32 devices in a mesh: rep: 2 (over x), data: 4 (over z), expert: 4 (over y, core).
Axes of the slice: x: 2, y: 2, z: 4, core: 2. Of those that a mesh axis runs over, the one named last changes fastest.
Arguments:
- x: bfloat16 [131072, 768], P(('rep', 'expert', 'data')), parts along dimension 0
- expert_idx: int32 [131072, 1], P(('rep', 'expert', 'data')), parts along dimension 0
- gate: float32 [131072, 1], P(('rep', 'expert', 'data')), parts along dimension 0
- w_gate: bfloat16 [8, 768, 3072], P('expert', 'data')
- w_up: bfloat16 [8, 768, 3072], P('expert', 'data')
- w_down: bfloat16 [8, 3072, 768], P('expert', None, 'data')
Outputs:
- output: bfloat16 [131072, 768], P(('rep', 'expert', 'data')), parts along dimension 0
There are 2 independent parts. The reference program is written for one: setup_inputs(seed, part) draws one part's arguments, and reference() takes and returns one part's arrays. A program takes and returns all parts, laid end to end along the dimension named above; an argument that names none is the same for every part.
All inputs are finite; a program needn't handle non-finite values.
Results may differ from the reference program's by a relative error of at most 0.001.
Values are sent between devices in bfloat16 or wider.
A program may use at most 1 GiB of HBM per device.

```python
import jax
import jax.numpy as jnp
from jax import lax

TOK_DEV = 4096
D_MODEL = 768
FFN = 3072
EXPERTS = 8
TOP_K = 1
EP_SIZE = 4
DP_SIZE = 4
CAPACITY = 640


def route_ids(key):
    n_blocks = EP_SIZE * DP_SIZE
    key_bias, key_hot, key_score = jax.random.split(key, 3)
    expert_bias = jax.random.randint(key_bias, (EXPERTS,), 0, 2 ** 20, dtype=jnp.int32)
    hot_expert = jax.random.randint(key_hot, (), 0, EXPERTS, dtype=jnp.int32)
    scores = jax.random.randint(key_score, (n_blocks, TOK_DEV, EXPERTS), 0, 2 ** 20, dtype=jnp.int32) + expert_bias
    forced = (jnp.arange(TOK_DEV) < CAPACITY)[None, :, None] & (jnp.arange(EXPERTS) == hot_expert)[None, None, :]
    scores = (scores + forced.astype(jnp.int32) * 2 ** 21) * EXPERTS + jnp.arange(EXPERTS, dtype=jnp.int32)
    chosen = lax.top_k(scores, TOP_K)[1]
    return chosen.reshape(n_blocks * TOK_DEV, TOP_K).astype(jnp.int32)


def setup_inputs(seed: int = 0, part: int = 0) -> dict:
    key_shared, key_local = jax.random.split(jax.random.key(seed))
    key_tok, key_route, key_gate = jax.random.split(jax.random.fold_in(key_local, part), 3)
    key_wg, key_wu, key_wd = jax.random.split(key_shared, 3)
    n_rows = EP_SIZE * DP_SIZE * TOK_DEV
    x = jax.random.normal(key_tok, (n_rows, D_MODEL), jnp.float32).astype(jnp.bfloat16)
    gate = jax.random.uniform(key_gate, (n_rows, TOP_K), jnp.float32, 0.2, 0.8)
    w_gate = (jax.random.normal(key_wg, (EXPERTS, D_MODEL, FFN), jnp.float32) * D_MODEL ** -0.5).astype(jnp.bfloat16)
    w_up = (jax.random.normal(key_wu, (EXPERTS, D_MODEL, FFN), jnp.float32) * D_MODEL ** -0.5).astype(jnp.bfloat16)
    w_down = (jax.random.normal(key_wd, (EXPERTS, FFN, D_MODEL), jnp.float32) * (1.5 * FFN ** -0.5)).astype(jnp.bfloat16)
    return {"x": x, "expert_idx": route_ids(key_route), "gate": gate, "w_gate": w_gate, "w_up": w_up, "w_down": w_down}


def slot_table(ids_flat):
    one_hot = (ids_flat[:, None] == jnp.arange(EXPERTS, dtype=jnp.int32)[None, :]).astype(jnp.int32)
    slot_ids = jnp.sum((jnp.cumsum(one_hot, axis=0) - one_hot) * one_hot, axis=1)
    return jnp.where(slot_ids < CAPACITY, ids_flat * CAPACITY + slot_ids, EXPERTS * CAPACITY)


def take_rows(block, index):
    return jnp.take(block, index, axis=0, mode="fill", fill_value=0)


def reference(x, expert_idx, gate, w_gate, w_up, w_down):
    n_blocks = EP_SIZE * DP_SIZE
    x_blocks = x.reshape(n_blocks, TOK_DEV, D_MODEL)
    dest_row = jax.vmap(slot_table)(expert_idx.reshape(n_blocks, TOK_DEV * TOP_K))
    block_ids = jnp.arange(n_blocks)[:, None]
    pair_token = jnp.broadcast_to(jnp.arange(TOK_DEV * TOP_K, dtype=jnp.int32) // TOP_K, dest_row.shape)
    src_tok = jnp.full((n_blocks, EXPERTS * CAPACITY), TOK_DEV, jnp.int32).at[block_ids, dest_row].set(pair_token, mode="drop")
    slot_gate = jnp.zeros((n_blocks, EXPERTS * CAPACITY), jnp.float32).at[block_ids, dest_row].set(gate.reshape(n_blocks, TOK_DEV * TOP_K), mode="drop")
    src_by_exp = src_tok.reshape(n_blocks, EXPERTS, CAPACITY).transpose(1, 0, 2)
    gate_by_exp = slot_gate.reshape(n_blocks, EXPERTS, CAPACITY).transpose(1, 0, 2)

    def expert_step(running, inputs):
        src_e, gate_e, wg_e, wu_e, wd_e = inputs
        expert_rows = jax.vmap(take_rows)(x_blocks, src_e).reshape(n_blocks * CAPACITY, D_MODEL)
        gate_act = jnp.dot(expert_rows, wg_e, preferred_element_type=jnp.float32)
        up_act = jnp.dot(expert_rows, wu_e, preferred_element_type=jnp.float32)
        hidden = (jax.nn.silu(gate_act) * up_act).astype(jnp.bfloat16)
        out_rows = jnp.dot(hidden, wd_e, preferred_element_type=jnp.float32).astype(jnp.bfloat16)
        contrib = out_rows.reshape(n_blocks, CAPACITY, D_MODEL).astype(jnp.float32) * gate_e[:, :, None]
        return running.at[block_ids, src_e].add(contrib, mode="drop"), None

    summed = lax.scan(expert_step, x_blocks.astype(jnp.float32), (src_by_exp, gate_by_exp, w_gate, w_up, w_down))[0]
    return summed.astype(jnp.bfloat16).reshape(n_blocks * TOK_DEV, D_MODEL)
```

```python
import jax
import jax.numpy as jnp
from jax import lax
from jax.sharding import PartitionSpec as P


def capacity_rows(tok_rows, top_k, n_exp):
    return max(8, ((5 * top_k * tok_rows) // (4 * n_exp) + 7) // 8 * 8)


def slot_table(ids_flat, n_exp, capacity):
    one_hot = (ids_flat[:, None] == jnp.arange(n_exp, dtype=jnp.int32)[None, :]).astype(jnp.int32)
    slot_ids = jnp.sum((jnp.cumsum(one_hot, axis=0) - one_hot) * one_hot, axis=1)
    return jnp.where(slot_ids < capacity, ids_flat * capacity + slot_ids, n_exp * capacity)


def dispatch_rows(x_loc, dest_row, n_slots, top_k):
    tok_rows = x_loc.shape[0]
    pair_token = jnp.arange(dest_row.shape[0], dtype=jnp.int32) // top_k
    src_tok = jnp.full((n_slots,), tok_rows, jnp.int32).at[dest_row].set(pair_token, mode="drop")
    return jnp.take(x_loc, src_tok, axis=0, mode="fill", fill_value=0)


def combine_rows(x_loc, gate_loc, back_rows, dest_row):
    tok_rows, d_model = x_loc.shape
    pair_out = jnp.take(back_rows, dest_row, axis=0, mode="fill", fill_value=0)
    mixed = jnp.sum(pair_out.reshape(tok_rows, gate_loc.shape[1], d_model) * gate_loc[:, :, None], axis=1)
    return (x_loc.astype(jnp.float32) + mixed).astype(jnp.bfloat16)


def expert_ffn(expert_rows, w_gate, w_up, w_down):
    gate_act = jnp.dot(expert_rows, w_gate, preferred_element_type=jnp.float32)
    up_act = jnp.dot(expert_rows, w_up, preferred_element_type=jnp.float32)
    hidden = (jax.nn.silu(gate_act) * up_act).astype(jnp.bfloat16)
    return jnp.dot(hidden, w_down, preferred_element_type=jnp.float32).astype(jnp.bfloat16)


def solution(mesh):
    n_rep, n_group = mesh.shape["rep"], mesh.shape["expert"]
    tok_spec = P(("rep", "expert", "data"), None)
    wide_spec = P("expert", "data", None)
    down_spec = P("expert", None, "data")

    def device_step(x_loc, idx_loc, gate_loc, wg_loc, wu_loc, wd_loc):
        tok_rows, d_model = x_loc.shape
        top_k = idx_loc.shape[1]
        n_exp = wg_loc.shape[0] * n_group
        capacity = capacity_rows(tok_rows, top_k, n_exp)
        mine = lax.axis_index("rep")
        wg_full = lax.all_gather(lax.dynamic_index_in_dim(wg_loc, mine, 0, False), "data", axis=0, tiled=True)
        wu_full = lax.all_gather(lax.dynamic_index_in_dim(wu_loc, mine, 0, False), "data", axis=0, tiled=True)
        wd_full = lax.all_gather(lax.dynamic_index_in_dim(wd_loc, mine, 0, False), "data", axis=1, tiled=True)
        dest_row = slot_table(idx_loc.reshape(tok_rows * top_k), n_exp, capacity)
        send_rows = dispatch_rows(x_loc, dest_row, n_exp * capacity, top_k).reshape(n_exp, capacity, d_model)
        recv_rows = lax.all_to_all(send_rows, ("expert", "rep"), 0, 0, tiled=True)
        out_rows = expert_ffn(recv_rows.reshape(n_exp * capacity, d_model), wg_full, wu_full, wd_full)
        back_rows = lax.all_to_all(out_rows.reshape(n_exp, capacity, d_model), ("expert", "rep"), 0, 0, tiled=True)
        return combine_rows(x_loc, gate_loc, back_rows.reshape(n_exp * capacity, d_model), dest_row)

    return jax.shard_map(device_step, mesh=mesh, in_specs=(tok_spec, tok_spec, tok_spec, wide_spec, wide_spec, down_spec), out_specs=tok_spec, check_vma=False)
```

```python
import functools

import jax
import jax.numpy as jnp
from jax import lax
from jax.experimental import pallas as pl
from jax.experimental.pallas import tpu as pltpu
from jax.sharding import PartitionSpec as P

MESH = pl.DeviceIdType.MESH
CHUNKS = 6
NZ = 4
PEERS = 8
LIGHT_AHEAD = 3
HEAVY_AHEAD = 2
VMEM_BYTES = 67_000_000


def capacity_rows(tok_rows, top_k, n_exp):
    return max(8, ((5 * top_k * tok_rows) // (4 * n_exp) + 7) // 8 * 8)


def moe_kernel(x_hbm, idx_ref, gate_ref, wg_hbm, wu_hbm, wd_hbm, out_hbm,
               wg_buf, wu_buf, wd_buf, wd_full, recv, sendb, back, acc, dest, dest_col, gate_col,
               w_recv, w_right, w_left, tok_recv, tok_send, ret_recv, ret_send, x_sem, go_sem, ready_sem):
    n_blk, blk = idx_ref.shape
    n_src, cap, d_model = recv.shape
    n_chunk, _, f_chunk = wg_buf.shape
    shard = d_model // NZ

    x = lax.axis_index("rep")
    z = lax.axis_index("data")
    p = lax.axis_index("expert")
    y, c = p // 2, p % 2
    me = 4 * y + 2 * c + x
    is_a = c == 0
    inner = jnp.logical_and(z > 0, z < NZ - 1)
    outer = jnp.logical_or(z == 0, z == NZ - 1)
    a_inner = jnp.logical_and(is_a, inner)

    def plane_id(dx, dy, cc):
        return (x + dx) % 2, (y + dy) % 2, cc

    def plane_dev(px, py, pc):
        return {"rep": px, "expert": 2 * py + pc}

    def plane_num(px, py, pc):
        return 4 * py + 2 * pc + px

    def w_view(j, s, m):
        if m == 0:
            return wg_buf.at[j, pl.ds(s * shard, shard), :]
        if m == 1:
            return wu_buf.at[j, pl.ds(s * shard, shard), :]
        return wd_buf.at[j, s]

    def w_local(j, m):
        if m == 2:
            src = wd_hbm.at[j]
        else:
            src = (wg_hbm, wu_hbm)[m].at[x, :, pl.ds(pl.multiple_of(j * f_chunk, f_chunk), f_chunk)]
        return pltpu.make_async_copy(src, w_view(j, z, m), w_recv.at[j, z, m])

    def w_send(j, s, m, right):
        view = w_view(j, s, m)
        return pltpu.make_async_remote_copy(
            src_ref=view, dst_ref=view,
            send_sem=(w_right if right else w_left).at[j, s, m], recv_sem=w_recv.at[j, s, m],
            device_id={"data": z + 1 if right else z - 1}, device_id_type=MESH)

    def own_start(j, right):
        for m in range(3):
            w_send(j, z, m, right).start()

    def own_light(j):
        @pl.when(z == 1)
        def _():
            own_start(j, True)

        @pl.when(z == 2)
        def _():
            own_start(j, False)

    def own_heavy(j):
        @pl.when(z == 1)
        def _():
            own_start(j, False)

        @pl.when(z == 2)
        def _():
            own_start(j, True)

    def own_outer():
        @pl.loop(0, n_chunk)
        def _(j):
            @pl.when(z == 0)
            def _():
                own_start(j, True)

            @pl.when(z == NZ - 1)
            def _():
                own_start(j, False)

    def event(j):
        @pl.when(jnp.logical_and(inner, j + LIGHT_AHEAD < n_chunk))
        def _():
            own_light(j + LIGHT_AHEAD)

        @pl.when(jnp.logical_and(inner, j + HEAVY_AHEAD < n_chunk))
        def _():
            own_heavy(j + HEAVY_AHEAD)

        for d in range(1, NZ):
            @pl.when(z - d >= 0)
            def _():
                for m in range(3):
                    w_send(j, z - d, m, True).wait_recv()

                    @pl.when(z < NZ - 1)
                    def _():
                        w_send(j, z - d, m, True).start()

            @pl.when(z + d < NZ)
            def _():
                for m in range(3):
                    w_send(j, z + d, m, False).wait_recv()

                    @pl.when(z > 0)
                    def _():
                        w_send(j, z + d, m, False).start()

    def wait_right(j):
        @pl.when(z < NZ - 1)
        def _():
            for d in range(NZ):
                @pl.when(z - d >= 0)
                def _():
                    for m in range(3):
                        w_send(j, z - d, m, True).wait_send()

    def wait_left(j):
        @pl.when(z > 0)
        def _():
            for d in range(NZ):
                @pl.when(z + d < NZ)
                def _():
                    for m in range(3):
                        w_send(j, z + d, m, False).wait_send()

    def go(right):
        @pl.loop(0, n_chunk - 1)
        def _(j):
            (wait_right if right else wait_left)(j)

        pl.semaphore_signal(go_sem.at[0 if right else 1], inc=1, device_id={"expert": p + 1}, device_id_type=MESH)

    def x_load(b, dst):
        return pltpu.make_async_copy(x_hbm.at[pl.ds(pl.multiple_of(b * blk, blk), blk), :], dst.at[b, pl.ds(0, blk), :], x_sem.at[b])

    @pl.loop(0, n_blk)
    def _(b):
        x_load(b, back).start()

    @pl.loop(0, n_chunk)
    def _(j):
        for m in range(3):
            w_local(j, m).start()

    barrier = pltpu.get_barrier_semaphore()
    for k in range(1, PEERS):
        dev = plane_dev(*plane_id(k % 2, (k // 2) % 2, (c + k // 4) % 2))
        pl.semaphore_signal(barrier, inc=1, device_id=dev, device_id_type=MESH)

    @pl.when(z > 0)
    def _():
        pl.semaphore_signal(barrier, inc=1, device_id={"data": z - 1}, device_id_type=MESH)

    @pl.when(z < NZ - 1)
    def _():
        pl.semaphore_signal(barrier, inc=1, device_id={"data": z + 1}, device_id_type=MESH)

    @pl.when(outer)
    def _():
        pl.semaphore_wait(barrier, PEERS)

    @pl.when(inner)
    def _():
        pl.semaphore_wait(barrier, PEERS + 1)

    @pl.loop(0, n_chunk)
    def _(j):
        for m in range(3):
            w_local(j, m).wait()

    @pl.when(is_a)
    def _():
        @pl.when(outer)
        def _():
            own_outer()

        @pl.when(inner)
        def _():
            for j in range(LIGHT_AHEAD):
                own_light(j)
            for j in range(HEAVY_AHEAD):
                own_heavy(j)

    tri = (lax.broadcasted_iota(jnp.int32, (blk, blk), 0) < lax.broadcasted_iota(jnp.int32, (blk, blk), 1)).astype(jnp.float32).astype(jnp.bfloat16)
    eye = lax.broadcasted_iota(jnp.int32, (blk, blk), 0) == lax.broadcasted_iota(jnp.int32, (blk, blk), 1)
    running = jnp.zeros((16, 1), jnp.float32)
    for b in range(n_blk):
        ids = idx_ref[b:b + 1, :]
        one_hot = (lax.broadcasted_iota(jnp.int32, (16, blk), 0) == ids).astype(jnp.float32)
        before = jnp.dot(one_hot.astype(jnp.bfloat16), tri, preferred_element_type=jnp.float32) + running
        slot = jnp.sum(one_hot * before, axis=0, keepdims=True)
        running = running + jnp.sum(one_hot, axis=1, keepdims=True)
        row = jnp.where(slot < cap, ids.astype(jnp.float32) * cap + slot, -1.0)
        dest[b:b + 1, :] = row.astype(jnp.int32)
        dest_col[b] = jnp.sum(jnp.where(eye, row, 0.0), axis=1, keepdims=True).astype(jnp.int32)
        gate_col[b] = jnp.sum(jnp.where(eye, gate_ref[b:b + 1, :], 0.0), axis=1, keepdims=True)

    @pl.loop(0, n_blk)
    def _(b):
        x_load(b, back).wait()

    def tok_copy(e, dev):
        return pltpu.make_async_remote_copy(
            src_ref=sendb.at[e], dst_ref=recv.at[me], send_sem=tok_send.at[e], recv_sem=tok_recv.at[me],
            device_id=dev, device_id_type=MESH)

    @pl.loop(0, PEERS)
    def _(k):
        kk = k % 4
        peer = plane_id((kk + 1) % 2, ((kk + 1) // 2) % 2, k // 4)
        e = plane_num(*peer)
        slots = lax.broadcasted_iota(jnp.int32, (cap, blk), 0) + e * cap

        def pick(b):
            hot = (slots == dest[pl.ds(b, 1), :]).astype(jnp.float32).astype(jnp.bfloat16)
            return jnp.dot(hot, back[b, 0:blk, :], preferred_element_type=jnp.float32)

        acc[0] = pick(0)

        @pl.loop(1, n_blk - 1)
        def _(b):
            acc[0] += pick(b)

        rows = (acc[0] + pick(n_blk - 1)).astype(jnp.bfloat16)

        @pl.when(e == me)
        def _():
            recv[me] = rows

        @pl.when(e != me)
        def _():
            sendb[e] = rows
            tok_copy(e, plane_dev(*peer)).start()

        for kq, ev in ((2, 0), (5, 1), (7, 2)):
            @pl.when(jnp.logical_and(a_inner, k == kq))
            def _():
                event(ev)

    for k in range(1, PEERS):
        dev = plane_dev(*plane_id(k % 2, (k // 2) % 2, (c + k // 4) % 2))
        pl.semaphore_signal(ready_sem, inc=1, device_id=dev, device_id_type=MESH)

    @pl.loop(0, n_src)
    def _(s):
        acc[s] = jnp.zeros((cap, d_model), jnp.float32)

    @pl.when(is_a)
    def _():
        @pl.when(inner)
        def _():
            @pl.loop(3, n_chunk)
            def _(j):
                event(j)

        @pl.when(z == 0)
        def _():
            go(True)

        @pl.when(z == NZ - 1)
        def _():
            go(False)

    @pl.when(c == 1)
    def _():
        @pl.when(z < 2)
        def _():
            pl.semaphore_wait(go_sem.at[0], 1)

        @pl.when(z >= 2)
        def _():
            pl.semaphore_wait(go_sem.at[1], 1)

        @pl.when(outer)
        def _():
            own_outer()

        @pl.when(inner)
        def _():
            for j in range(LIGHT_AHEAD):
                own_light(j)

            @pl.when(z == 1)
            def _():
                pl.semaphore_wait(go_sem.at[1], 1)

            @pl.when(z == 2)
            def _():
                pl.semaphore_wait(go_sem.at[0], 1)

            for j in range(HEAVY_AHEAD):
                own_heavy(j)
            event(0)
            event(1)

    for k in range(1, PEERS):
        peer = plane_id(k % 2, (k // 2) % 2, (c + k // 4) % 2)
        s = plane_num(*peer)
        pltpu.make_async_remote_copy(
            src_ref=sendb.at[s], dst_ref=recv.at[s], send_sem=tok_send.at[s], recv_sem=tok_recv.at[s],
            device_id=plane_dev(*peer), device_id_type=MESH).wait_recv()

    def load_down(j):
        for s in range(NZ):
            piece = wd_buf[j, s]
            wd_full[0:f_chunk // 2, s * shard:(s + 1) * shard] = piece[:, :shard]
            wd_full[f_chunk // 2:f_chunk, s * shard:(s + 1) * shard] = piece[:, shard:]

    def ffn(j, s):
        rows = recv[s]
        g = jnp.dot(rows, wg_buf[j], preferred_element_type=jnp.float32)
        u = jnp.dot(rows, wu_buf[j], preferred_element_type=jnp.float32)
        h = (g * jax.nn.sigmoid(g) * u).astype(jnp.bfloat16)
        return jnp.dot(h, wd_full[...], preferred_element_type=jnp.float32)

    def before_chunk(j):
        @pl.when(outer)
        def _():
            event(j)

        @pl.when(jnp.logical_and(jnp.logical_and(c == 1, inner), j + 2 < n_chunk))
        def _():
            event(j + 2)

        load_down(j)

    @pl.loop(0, n_chunk - 1)
    def _(j):
        before_chunk(j)

        @pl.loop(0, n_src)
        def _(s):
            acc[s] += ffn(j, s)

        @pl.when(jnp.logical_and(a_inner, j == 0))
        def _():
            @pl.when(z == 1)
            def _():
                go(True)

            @pl.when(z == 2)
            def _():
                go(False)

        @pl.when(jnp.logical_and(a_inner, j == 1))
        def _():
            @pl.when(z == 1)
            def _():
                go(False)

            @pl.when(z == 2)
            def _():
                go(True)

    before_chunk(n_chunk - 1)
    for k in range(1, PEERS):
        peer = plane_id(k % 2, (k // 2) % 2, (c + k // 4) % 2)
        tok_copy(plane_num(*peer), plane_dev(*peer)).wait_send()
    pl.semaphore_wait(ready_sem, PEERS - 1)

    def ret_copy(s, dev):
        return pltpu.make_async_remote_copy(
            src_ref=sendb.at[s], dst_ref=back.at[me], send_sem=ret_send.at[s], recv_sem=ret_recv.at[me],
            device_id=dev, device_id_type=MESH)

    @pl.loop(0, PEERS)
    def _(r):
        q, rr = r // 4, r % 4
        peer = plane_id((1 - q) * ((rr + 1) % 2) + q * (1 - rr // 2), (1 - q) * (rr % 2) + q * (1 - rr // 2), (c + rr // 2 + q * rr) % 2)
        s = plane_num(*peer)
        rows = (acc[s] + ffn(n_chunk - 1, s)).astype(jnp.bfloat16)

        @pl.when(s == me)
        def _():
            back[me] = rows

        @pl.when(s != me)
        def _():
            sendb[s] = rows
            ret_copy(s, plane_dev(*peer)).start()

    @pl.loop(0, n_blk)
    def _(b):
        x_load(b, recv).start()

    @pl.loop(0, n_blk)
    def _(b):
        acc[b, 0:blk, :] = jnp.zeros((blk, d_model), jnp.float32)

    def arrived(k):
        kk = k % 4
        peer = plane_id((kk // 2 + kk + 1) % 2, kk % 2, k // 4)
        e = plane_num(*peer)

        @pl.when(e != me)
        def _():
            pltpu.make_async_remote_copy(
                src_ref=sendb.at[e], dst_ref=back.at[e], send_sem=ret_send.at[e], recv_sem=ret_recv.at[e],
                device_id=plane_dev(*peer), device_id_type=MESH).wait_recv()

        return e

    def put_back(e, b):
        hot = (lax.broadcasted_iota(jnp.int32, (blk, cap), 1) + e * cap == dest_col[b]).astype(jnp.float32).astype(jnp.bfloat16)
        return jnp.dot(hot, back[e], preferred_element_type=jnp.float32)

    @pl.loop(0, PEERS - 1)
    def _(k):
        e = arrived(k)

        @pl.loop(0, n_blk)
        def _(b):
            acc[b, 0:blk, :] += put_back(e, b)

    @pl.loop(0, n_blk)
    def _(b):
        x_load(b, recv).wait()

    e_last = arrived(PEERS - 1)

    def out_copy(b):
        return pltpu.make_async_copy(recv.at[b, pl.ds(0, blk), :], out_hbm.at[pl.ds(pl.multiple_of(b * blk, blk), blk), :], x_sem.at[b])

    @pl.loop(0, n_blk)
    def _(b):
        mixed = (acc[b, 0:blk, :] + put_back(e_last, b)) * gate_col[b]
        recv[b, 0:blk, :] = (recv[b, 0:blk, :].astype(jnp.float32) + mixed).astype(jnp.bfloat16)
        out_copy(b).start()

    @pl.when(is_a)
    def _():
        wait_right(n_chunk - 1)
        wait_left(n_chunk - 1)

    @pl.when(c == 1)
    def _():
        @pl.loop(0, n_chunk)
        def _(j):
            wait_right(j)
            wait_left(j)

    for k in range(1, PEERS):
        peer = plane_id(k % 2, (k // 2) % 2, (c + k // 4) % 2)
        ret_copy(plane_num(*peer), plane_dev(*peer)).wait_send()

    @pl.loop(0, n_blk)
    def _(b):
        out_copy(b).wait()


def solution(mesh):
    n_group = mesh.shape["expert"]
    tok_spec = P(("rep", "expert", "data"), None)
    wide_spec = P("expert", "data", None)
    down_spec = P("expert", None, "data")

    def device_step(x_loc, idx_loc, gate_loc, wg_loc, wu_loc, wd_loc):
        tok_rows, d_model = x_loc.shape
        top_k = idx_loc.shape[1]
        n_exp = wg_loc.shape[0] * n_group
        ffn = wg_loc.shape[2]
        cap = capacity_rows(tok_rows, top_k, n_exp)
        blk = tok_rows // PEERS
        f_chunk = ffn // CHUNKS
        shard = d_model // NZ
        wd_own = lax.dynamic_index_in_dim(wd_loc, lax.axis_index("rep"), 0, False)
        wd_own = wd_own.reshape(CHUNKS, 2, f_chunk // 2, shard).transpose(0, 2, 1, 3).reshape(CHUNKS, f_chunk // 2, 2 * shard)
        any_spec = pl.BlockSpec(memory_space=pl.ANY)
        vmem_spec = pl.BlockSpec(memory_space=pltpu.VMEM)
        dma = pltpu.SemaphoreType.DMA
        return pl.pallas_call(
            moe_kernel,
            out_shape=jax.ShapeDtypeStruct((tok_rows, d_model), jnp.bfloat16),
            in_specs=[any_spec, vmem_spec, vmem_spec, any_spec, any_spec, any_spec],
            out_specs=any_spec,
            scratch_shapes=[
                pltpu.VMEM((CHUNKS, d_model, f_chunk), jnp.bfloat16),
                pltpu.VMEM((CHUNKS, d_model, f_chunk), jnp.bfloat16),
                pltpu.VMEM((CHUNKS, NZ, f_chunk // 2, 2 * shard), jnp.bfloat16),
                pltpu.VMEM((f_chunk, d_model), jnp.bfloat16),
                pltpu.VMEM((PEERS, cap, d_model), jnp.bfloat16),
                pltpu.VMEM((PEERS, cap, d_model), jnp.bfloat16),
                pltpu.VMEM((PEERS, cap, d_model), jnp.bfloat16),
                pltpu.VMEM((PEERS, cap, d_model), jnp.float32),
                pltpu.VMEM((PEERS, blk), jnp.int32),
                pltpu.VMEM((PEERS, blk, 1), jnp.int32),
                pltpu.VMEM((PEERS, blk, 1), jnp.float32),
                dma((CHUNKS, NZ, 3)), dma((CHUNKS, NZ, 3)), dma((CHUNKS, NZ, 3)),
                dma((PEERS,)), dma((PEERS,)), dma((PEERS,)), dma((PEERS,)), dma((PEERS,)),
                pltpu.SemaphoreType.REGULAR((2,)), pltpu.SemaphoreType.REGULAR,
            ],
            compiler_params=pltpu.CompilerParams(collective_id=0, has_side_effects=True, vmem_limit_bytes=VMEM_BYTES),
        )(x_loc, idx_loc.reshape(PEERS, blk), gate_loc.reshape(PEERS, blk), wg_loc, wu_loc, wd_own)

    return jax.shard_map(device_step, mesh=mesh, in_specs=(tok_spec, tok_spec, tok_spec, wide_spec, wide_spec, down_spec), out_specs=tok_spec, check_vma=False)
```

```python
import functools

import jax
import jax.numpy as jnp
from jax import lax
from jax.experimental import pallas as pl
from jax.experimental.pallas import tpu as pltpu
from jax.sharding import PartitionSpec as P

MESH = pl.DeviceIdType.MESH
CHUNKS = 6
NZ = 4
PEERS = 8
AHEAD = 3
VMEM_BYTES = 67_000_000


def capacity_rows(tok_rows, top_k, n_exp):
    return max(8, ((5 * top_k * tok_rows) // (4 * n_exp) + 7) // 8 * 8)


def moe_kernel(x_hbm, idx_ref, gate_ref, wg_hbm, wu_hbm, wd_hbm, out_hbm,
               wg_buf, wu_buf, wd_buf, recv, sendb, back, acc, dest, dest_col, gate_col,
               w_recv, w_light, w_heavy, tok_recv, tok_send, ret_recv, ret_send, x_sem, go_sem, ready_sem):
    n_src, cap, d_model = recv.shape
    n_blk, _, _ = dest_col.shape
    blk = dest_col.shape[1]
    n_chunk, _, f_chunk = wg_buf.shape
    shard = d_model // NZ

    x = lax.axis_index("rep")
    z = lax.axis_index("data")
    p = lax.axis_index("expert")
    y, c = p // 2, p % 2
    me = 4 * c + 2 * y + x
    is_a = c == 0
    inner = jnp.logical_and(z > 0, z < NZ - 1)
    outer = jnp.logical_or(z == 0, z == NZ - 1)
    a_inner = jnp.logical_and(is_a, inner)

    def plane_id(dx, dy, cc):
        return (x + dx) % 2, (y + dy) % 2, cc

    def plane_dev(px, py, pc):
        return {"rep": px, "expert": 2 * py + pc}

    def plane_num(px, py, pc):
        return 4 * pc + 2 * py + px

    def w_view(j, s, m):
        return (wg_buf, wu_buf, wd_buf)[m].at[j, pl.ds(s * shard, shard), :]

    def w_local(j, m):
        src = (wg_hbm, wu_hbm, wd_hbm)[m].at[x, :, pl.ds(pl.multiple_of(j * f_chunk, f_chunk), f_chunk)]
        return pltpu.make_async_copy(src, w_view(j, z, m), w_recv.at[j, z, m])

    def w_copy(j, s, m, heavy, dev):
        view = w_view(j, s, m)
        return pltpu.make_async_remote_copy(
            src_ref=view, dst_ref=view, send_sem=(w_heavy if heavy else w_light).at[j, s, m], recv_sem=w_recv.at[j, s, m],
            device_id={"data": dev}, device_id_type=MESH)

    end, far, mate = 3 * (z - 1), 3 * (2 - z), 3 - z

    def pass_on(j, s, heavy, arrives=True):
        for m in range(3):
            cp = w_copy(j, s, m, heavy, end if heavy else mate)
            if arrives:
                cp.wait_recv()
            cp.start()

    def light_own(j):
        pass_on(j, z, False, False)

    def light_end(j):
        pass_on(j, end, False)

    def heavy_own(j):
        pass_on(j, z, True, False)

    def heavy_mate(j):
        pass_on(j, mate, True)

    def heavy_far(j):
        pass_on(j, far, True)

    def heavy_all(j):
        heavy_own(j)
        heavy_mate(j)
        heavy_far(j)

    def own_outer():
        @pl.loop(0, n_chunk)
        def _(j):
            for m in range(3):
                w_copy(j, z, m, False, (z + 3) // 3).start()

    def end_wait(j):
        for d in range(1, NZ):
            for m in range(3):
                w_copy(j, (z + d) % NZ, m, False, (z + 3) // 3).wait_recv()

    def sent(j, shards, heavy):
        for s in shards:
            for m in range(3):
                w_copy(j, s, m, heavy, (z + 1) % NZ).wait_send()

    def sent_outer(j):
        sent(j, (z,), False)

    def sent_light(j):
        sent(j, (z, end), False)

    def sent_heavy(j):
        sent(j, (z, mate, far), True)

    def go(done, heavy):
        @pl.loop(0, n_chunk - 1)
        def _(j):
            done(j)

        pl.semaphore_signal(go_sem.at[heavy], inc=1, device_id={"expert": p + 1}, device_id_type=MESH)

    def x_load(b, dst):
        return pltpu.make_async_copy(x_hbm.at[pl.ds(pl.multiple_of(b * blk, blk), blk), :], dst.at[b, pl.ds(0, blk), :], x_sem.at[b])

    @pl.loop(0, n_blk)
    def _(b):
        x_load(b, back).start()

    @pl.loop(0, n_chunk)
    def _(j):
        for m in range(3):
            w_local(j, m).start()

    barrier = pltpu.get_barrier_semaphore()
    for k in range(1, PEERS):
        dev = plane_dev(*plane_id(k % 2, (k // 2) % 2, (c + k // 4) % 2))
        pl.semaphore_signal(barrier, inc=1, device_id=dev, device_id_type=MESH)

    @pl.when(z > 0)
    def _():
        pl.semaphore_signal(barrier, inc=1, device_id={"data": z - 1}, device_id_type=MESH)

    @pl.when(z < NZ - 1)
    def _():
        pl.semaphore_signal(barrier, inc=1, device_id={"data": z + 1}, device_id_type=MESH)

    @pl.when(outer)
    def _():
        pl.semaphore_wait(barrier, PEERS)

    @pl.when(inner)
    def _():
        pl.semaphore_wait(barrier, PEERS + 1)

    @pl.loop(0, n_chunk)
    def _(j):
        for m in range(3):
            w_local(j, m).wait()

    @pl.when(is_a)
    def _():
        @pl.when(outer)
        def _():
            own_outer()

        @pl.when(inner)
        def _():
            for j in range(AHEAD):
                light_own(j)
                heavy_own(j)

    tri = (lax.broadcasted_iota(jnp.int32, (blk, blk), 0) < lax.broadcasted_iota(jnp.int32, (blk, blk), 1)).astype(jnp.float32).astype(jnp.bfloat16)
    eye = lax.broadcasted_iota(jnp.int32, (blk, blk), 0) == lax.broadcasted_iota(jnp.int32, (blk, blk), 1)
    running = jnp.zeros((16, 1), jnp.float32)
    for b in range(n_blk):
        ids = idx_ref[:, b * blk:(b + 1) * blk]
        ids = (ids // 2 % 2) * 4 + (ids // 4) * 2 + ids % 2
        one_hot = (lax.broadcasted_iota(jnp.int32, (16, blk), 0) == ids).astype(jnp.float32)
        before = jnp.dot(one_hot.astype(jnp.bfloat16), tri, preferred_element_type=jnp.float32) + running
        slot = jnp.sum(one_hot * before, axis=0, keepdims=True)
        running = running + jnp.sum(one_hot, axis=1, keepdims=True)
        row = jnp.where(slot < cap, ids.astype(jnp.float32) * cap + slot, -1.0)
        dest[b:b + 1, :] = row.astype(jnp.int32)
        dest_col[b] = jnp.sum(jnp.where(eye, row, 0.0), axis=1, keepdims=True).astype(jnp.int32)
        gate_col[b] = jnp.sum(jnp.where(eye, gate_ref[:, b * blk:(b + 1) * blk], 0.0), axis=1, keepdims=True)

    @pl.loop(0, n_blk)
    def _(b):
        x_load(b, back).wait()

    def tok_copy(e, dev):
        return pltpu.make_async_remote_copy(
            src_ref=sendb.at[e], dst_ref=recv.at[me], send_sem=tok_send.at[e], recv_sem=tok_recv.at[me],
            device_id=dev, device_id_type=MESH)

    @pl.loop(0, PEERS)
    def _(k):
        kk = k % 4
        peer = plane_id((kk + 1) % 2, ((kk + 1) // 2) % 2, k // 4)
        e = plane_num(*peer)
        slots = lax.broadcasted_iota(jnp.int32, (cap, blk), 0) + e * cap

        def pick(b):
            hot = (slots == dest[pl.ds(b, 1), :]).astype(jnp.float32).astype(jnp.bfloat16)
            return jnp.dot(hot, back[b, 0:blk, :], preferred_element_type=jnp.float32)

        acc[0] = pick(0)

        @pl.loop(1, n_blk - 1)
        def _(b):
            acc[0] += pick(b)

        rows = (acc[0] + pick(n_blk - 1)).astype(jnp.bfloat16)

        @pl.when(e == me)
        def _():
            recv[me] = rows

        @pl.when(e != me)
        def _():
            sendb[e] = rows
            tok_copy(e, plane_dev(*peer)).start()

        def at(step):
            return pl.when(jnp.logical_and(a_inner, k == step))

        @at(1)
        def _():
            light_end(0)
            light_own(3)

        @at(2)
        def _():
            light_end(1)
            light_own(4)
            heavy_mate(0)
            heavy_mate(1)
            heavy_own(3)

        @at(3)
        def _():
            light_end(2)
            light_own(5)

        @at(4)
        def _():
            light_end(3)
            heavy_mate(2)
            heavy_far(0)
            heavy_own(4)

        @at(5)
        def _():
            light_end(4)

        @at(6)
        def _():
            light_end(5)
            heavy_mate(3)
            heavy_far(1)
            heavy_own(5)

        @pl.when(jnp.logical_and(jnp.logical_and(is_a, outer), k == 6))
        def _():
            go(sent_outer, 0)

    for k in range(1, PEERS):
        dev = plane_dev(*plane_id(k % 2, (k // 2) % 2, (c + k // 4) % 2))
        pl.semaphore_signal(ready_sem, inc=1, device_id=dev, device_id_type=MESH)

    @pl.loop(0, n_src)
    def _(s):
        acc[s] = jnp.zeros((cap, d_model), jnp.float32)

    @pl.when(a_inner)
    def _():
        heavy_mate(4)
        heavy_far(2)

    @pl.when(c == 1)
    def _():
        pl.semaphore_wait(go_sem.at[0], 1)

        @pl.when(outer)
        def _():
            own_outer()

        @pl.when(inner)
        def _():
            @pl.loop(0, n_chunk)
            def _(j):
                light_own(j)
                light_end(j)

            pl.semaphore_wait(go_sem.at[1], 1)

            @pl.loop(0, 3)
            def _(j):
                heavy_all(j)

    for k in range(1, PEERS):
        peer = plane_id(k % 2, (k // 2) % 2, (c + k // 4) % 2)
        s = plane_num(*peer)
        pltpu.make_async_remote_copy(
            src_ref=sendb.at[s], dst_ref=recv.at[s], send_sem=tok_send.at[s], recv_sem=tok_recv.at[s],
            device_id=plane_dev(*peer), device_id_type=MESH).wait_recv()

    @pl.when(a_inner)
    def _():
        heavy_mate(5)

    def ffn(j, s):
        rows = recv[s]
        g = jnp.dot(rows, wg_buf[j], preferred_element_type=jnp.float32)
        u = jnp.dot(rows, wu_buf[j], preferred_element_type=jnp.float32)
        h = (g * jax.nn.sigmoid(g) * u).astype(jnp.bfloat16)
        return lax.dot_general(h, wd_buf[j], (((1,), (1,)), ((), ())), preferred_element_type=jnp.float32)

    def before_chunk(j):
        @pl.when(outer)
        def _():
            end_wait(j)

    @pl.loop(0, n_chunk - 1)
    def _(j):
        before_chunk(j)

        @pl.loop(0, n_src)
        def _(s):
            acc[s] += ffn(j, s)

        @pl.when(jnp.logical_and(a_inner, j == 0))
        def _():
            heavy_far(3)
            heavy_far(4)
            go(sent_light, 0)

        @pl.when(jnp.logical_and(a_inner, j == 1))
        def _():
            heavy_far(5)

        @pl.when(jnp.logical_and(a_inner, j == 2))
        def _():
            go(sent_heavy, 1)

        @pl.when(jnp.logical_and(jnp.logical_and(c == 1, inner), j < 3))
        def _():
            heavy_all(j + 3)

    before_chunk(n_chunk - 1)
    for k in range(1, PEERS):
        peer = plane_id(k % 2, (k // 2) % 2, (c + k // 4) % 2)
        tok_copy(plane_num(*peer), plane_dev(*peer)).wait_send()
    pl.semaphore_wait(ready_sem, PEERS - 1)

    def ret_copy(s, dev):
        return pltpu.make_async_remote_copy(
            src_ref=sendb.at[s], dst_ref=back.at[me], send_sem=ret_send.at[s], recv_sem=ret_recv.at[me],
            device_id=dev, device_id_type=MESH)

    @pl.loop(0, PEERS)
    def _(r):
        q, rr = r // 4, r % 4
        peer = plane_id((1 - q) * ((rr + 1) % 2) + q * (1 - rr // 2), (1 - q) * (rr % 2) + q * (1 - rr // 2), (c + rr // 2 + q * rr) % 2)
        s = plane_num(*peer)
        rows = (acc[s] + ffn(n_chunk - 1, s)).astype(jnp.bfloat16)

        @pl.when(s == me)
        def _():
            back[me] = rows

        @pl.when(s != me)
        def _():
            sendb[s] = rows
            ret_copy(s, plane_dev(*peer)).start()

    @pl.loop(0, n_blk)
    def _(b):
        x_load(b, recv).start()

    @pl.loop(0, n_blk)
    def _(b):
        acc[b, 0:blk, :] = jnp.zeros((blk, d_model), jnp.float32)

    def arrived(k):
        py, pc = (y + k) % 2, k // 2
        for dx in range(2):
            peer = ((x + dx) % 2, py, pc)
            e = plane_num(*peer)

            @pl.when(e != me)
            def _():
                pltpu.make_async_remote_copy(
                    src_ref=sendb.at[e], dst_ref=back.at[e], send_sem=ret_send.at[e], recv_sem=ret_recv.at[e],
                    device_id=plane_dev(*peer), device_id_type=MESH).wait_recv()

        return 4 * pc + 2 * py

    def put_back(e, b):
        hot = (lax.broadcasted_iota(jnp.int32, (blk, 2 * cap), 1) + e * cap == dest_col[b]).astype(jnp.float32).astype(jnp.bfloat16)
        rows = back[pl.ds(e, 2)].reshape(2 * cap, d_model)
        return jnp.dot(hot, rows, preferred_element_type=jnp.float32)

    @pl.loop(0, PEERS // 2 - 1)
    def _(k):
        e = arrived(k)

        @pl.loop(0, n_blk)
        def _(b):
            acc[b, 0:blk, :] += put_back(e, b)

    @pl.loop(0, n_blk)
    def _(b):
        x_load(b, recv).wait()

    e_last = arrived(PEERS // 2 - 1)

    def out_copy(b):
        return pltpu.make_async_copy(recv.at[b, pl.ds(0, blk), :], out_hbm.at[pl.ds(pl.multiple_of(b * blk, blk), blk), :], x_sem.at[b])

    @pl.loop(0, n_blk)
    def _(b):
        mixed = (acc[b, 0:blk, :] + put_back(e_last, b)) * gate_col[b]
        recv[b, 0:blk, :] = (recv[b, 0:blk, :].astype(jnp.float32) + mixed).astype(jnp.bfloat16)
        out_copy(b).start()

    @pl.loop((n_chunk - 1) * (1 - c), n_chunk)
    def _(j):
        @pl.when(outer)
        def _():
            sent_outer(j)

        @pl.when(inner)
        def _():
            sent_light(j)
            sent_heavy(j)

    for k in range(1, PEERS):
        peer = plane_id(k % 2, (k // 2) % 2, (c + k // 4) % 2)
        ret_copy(plane_num(*peer), plane_dev(*peer)).wait_send()

    @pl.loop(0, n_blk)
    def _(b):
        out_copy(b).wait()


def solution(mesh):
    n_group = mesh.shape["expert"]
    tok_spec = P(("rep", "expert", "data"), None)
    wide_spec = P("expert", "data", None)
    down_spec = P("expert", None, "data")

    def device_step(x_loc, idx_loc, gate_loc, wg_loc, wu_loc, wd_loc):
        tok_rows, d_model = x_loc.shape
        top_k = idx_loc.shape[1]
        n_exp = wg_loc.shape[0] * n_group
        ffn = wg_loc.shape[2]
        cap = capacity_rows(tok_rows, top_k, n_exp)
        blk = tok_rows // PEERS
        f_chunk = ffn // CHUNKS
        any_spec = pl.BlockSpec(memory_space=pl.ANY)
        vmem_spec = pl.BlockSpec(memory_space=pltpu.VMEM)
        dma = pltpu.SemaphoreType.DMA
        return pl.pallas_call(
            moe_kernel,
            out_shape=jax.ShapeDtypeStruct((tok_rows, d_model), jnp.bfloat16),
            in_specs=[any_spec, vmem_spec, vmem_spec, any_spec, any_spec, any_spec],
            out_specs=any_spec,
            scratch_shapes=[
                pltpu.VMEM((CHUNKS, d_model, f_chunk), jnp.bfloat16),
                pltpu.VMEM((CHUNKS, d_model, f_chunk), jnp.bfloat16),
                pltpu.VMEM((CHUNKS, d_model, f_chunk), jnp.bfloat16),
                pltpu.VMEM((PEERS, cap, d_model), jnp.bfloat16),
                pltpu.VMEM((PEERS, cap, d_model), jnp.bfloat16),
                pltpu.VMEM((PEERS, cap, d_model), jnp.bfloat16),
                pltpu.VMEM((PEERS, cap, d_model), jnp.float32),
                pltpu.VMEM((PEERS, blk), jnp.int32),
                pltpu.VMEM((PEERS, blk, 1), jnp.int32),
                pltpu.VMEM((PEERS, blk, 1), jnp.float32),
                dma((CHUNKS, NZ, 3)), dma((CHUNKS, NZ, 3)), dma((CHUNKS, NZ, 3)),
                dma((PEERS,)), dma((PEERS,)), dma((PEERS,)), dma((PEERS,)), dma((PEERS,)),
                pltpu.SemaphoreType.REGULAR((2,)), pltpu.SemaphoreType.REGULAR,
            ],
            compiler_params=pltpu.CompilerParams(collective_id=0, has_side_effects=True, vmem_limit_bytes=VMEM_BYTES),
        )(x_loc, idx_loc.T, gate_loc.T, wg_loc, wu_loc, wd_loc.transpose(0, 2, 1))

    return jax.shard_map(device_step, mesh=mesh, in_specs=(tok_spec, tok_spec, tok_spec, wide_spec, wide_spec, down_spec), out_specs=tok_spec, check_vma=False)
```

```python
import functools

import jax
import jax.numpy as jnp
from jax import lax
from jax.experimental import pallas as pl
from jax.experimental.pallas import tpu as pltpu
from jax.sharding import PartitionSpec as P

MESH = pl.DeviceIdType.MESH
CHUNKS = 6
NZ = 4
PEERS = 8
AHEAD = 3
VMEM_BYTES = 67_000_000


def capacity_rows(tok_rows, top_k, n_exp):
    return max(8, ((5 * top_k * tok_rows) // (4 * n_exp) + 7) // 8 * 8)


def low_rows(cap):
    return cap * 3 // 5 // 8 * 8


def moe_kernel(x_hbm, idx_ref, gate_ref, wg_hbm, wu_hbm, wd_hbm, out_hbm, relay_hbm,
               wg_buf, wu_buf, wd_buf, recv, sendb, back, acc, x_buf, dest, cols,
               w_recv, w_light, w_heavy, tok_recv, tok_send, ret_recv, ret_send, relay_recv, relay_send, fwd_send,
               x_sem, out_sem, go_sem, ready_sem):
    n_src, cap, d_model = back.shape
    low = low_rows(cap)
    n_blk, blk, _ = cols.shape
    n_chunk, _, f_chunk = wg_buf.shape
    shard = d_model // NZ

    x = lax.axis_index("rep")
    z = lax.axis_index("data")
    p = lax.axis_index("expert")
    y, c = p // 2, p % 2
    me = 4 * c + 2 * y + x
    is_a = c == 0
    inner = jnp.logical_and(z > 0, z < NZ - 1)
    outer = jnp.logical_or(z == 0, z == NZ - 1)
    is_b = c == 1
    a_inner = jnp.logical_and(is_a, inner)
    b_inner = jnp.logical_and(is_b, inner)
    b_outer = jnp.logical_and(is_b, outer)
    inward = (z + 3) // 3

    def plane_id(dx, dy, cc):
        return (x + dx) % 2, (y + dy) % 2, cc

    def plane_dev(px, py, pc):
        return {"rep": px, "expert": 2 * py + pc}

    def plane_num(px, py, pc):
        return 4 * pc + 2 * py + px

    def w_view(j, s, m):
        return (wg_buf, wu_buf, wd_buf)[m].at[j, pl.ds(s * shard, shard), :]

    def w_local(j, m):
        src = (wg_hbm, wu_hbm, wd_hbm)[m].at[x, :, pl.ds(pl.multiple_of(j * f_chunk, f_chunk), f_chunk)]
        return pltpu.make_async_copy(src, w_view(j, z, m), w_recv.at[j, z, m])

    def w_copy(j, s, m, heavy, dev):
        view = w_view(j, s, m)
        return pltpu.make_async_remote_copy(
            src_ref=view, dst_ref=view, send_sem=(w_heavy if heavy else w_light).at[j, s, m], recv_sem=w_recv.at[j, s, m],
            device_id={"data": dev}, device_id_type=MESH)

    end, far, mate = 3 * (z - 1), 3 * (2 - z), 3 - z

    def pass_on(j, s, heavy, arrives=True):
        for m in range(3):
            cp = w_copy(j, s, m, heavy, end if heavy else mate)
            if arrives:
                cp.wait_recv()
            cp.start()

    def light_own(j):
        pass_on(j, z, False, False)

    def light_end(j):
        pass_on(j, end, False)

    def heavy_own(j):
        pass_on(j, z, True, False)

    def heavy_mate(j):
        pass_on(j, mate, True)

    def heavy_far(j):
        pass_on(j, far, True)

    def heavy_all(j):
        heavy_own(j)
        heavy_mate(j)
        heavy_far(j)

    def own_outer():
        @pl.loop(0, n_chunk)
        def _(j):
            for m in range(3):
                w_copy(j, z, m, False, inward).start()

    def end_wait(j):
        for d in range(1, NZ):
            for m in range(3):
                w_copy(j, (z + d) % NZ, m, False, inward).wait_recv()

    def sent(j, shards, heavy):
        for s in shards:
            for m in range(3):
                w_copy(j, s, m, heavy, (z + 1) % NZ).wait_send()

    def sent_outer(j):
        sent(j, (z,), False)

    def sent_light(j):
        sent(j, (z, end), False)

    def sent_heavy(j):
        sent(j, (z, mate, far), True)

    def go(done, heavy):
        @pl.loop(0, n_chunk - 1)
        def _(j):
            done(j)

        pl.semaphore_signal(go_sem.at[heavy], inc=1, device_id={"expert": p + 1}, device_id_type=MESH)

    def x_rows(ref, b):
        return ref.at[pl.ds(pl.multiple_of(b * blk, blk), blk), :]

    def x_load(b):
        return pltpu.make_async_copy(x_rows(x_hbm, b), back.at[b, pl.ds(0, blk), :], x_sem.at[b])

    half = blk // 2

    def x_again(b, h):
        rows = pl.ds(pl.multiple_of(b * blk + h * half, half), half)
        return pltpu.make_async_copy(x_hbm.at[rows, :], x_buf.at[h], x_sem.at[h])

    @pl.loop(0, n_chunk)
    def _(j):
        for m in range(3):
            w_local(j, m).start()

    @pl.loop(0, n_blk)
    def _(b):
        x_load(b).start()

    barrier = pltpu.get_barrier_semaphore()
    for k in range(1, PEERS):
        dev = plane_dev(*plane_id(k % 2, (k // 2) % 2, (c + k // 4) % 2))
        pl.semaphore_signal(barrier, inc=1, device_id=dev, device_id_type=MESH)

    @pl.when(z > 0)
    def _():
        pl.semaphore_signal(barrier, inc=1, device_id={"data": z - 1}, device_id_type=MESH)

    @pl.when(z < NZ - 1)
    def _():
        pl.semaphore_signal(barrier, inc=1, device_id={"data": z + 1}, device_id_type=MESH)

    @pl.when(b_inner)
    def _():
        for cc in range(2):
            dev = {"rep": 1 - x, "data": end, "expert": 2 * (1 - y) + cc}
            pl.semaphore_signal(barrier, inc=1, device_id=dev, device_id_type=MESH)

    pl.semaphore_wait(barrier, PEERS + 1)

    @pl.loop(0, n_chunk)
    def _(j):
        for m in range(3):
            w_local(j, m).wait()

    @pl.when(is_a)
    def _():
        @pl.when(outer)
        def _():
            own_outer()

        @pl.when(inner)
        def _():
            for j in range(AHEAD):
                light_own(j)
                heavy_own(j)

    tri = (lax.broadcasted_iota(jnp.int32, (blk, blk), 0) < lax.broadcasted_iota(jnp.int32, (blk, blk), 1)).astype(jnp.float32).astype(jnp.bfloat16)
    eye = lax.broadcasted_iota(jnp.int32, (blk, blk), 0) == lax.broadcasted_iota(jnp.int32, (blk, blk), 1)
    running = jnp.zeros((16, 1), jnp.float32)
    for b in range(n_blk):
        ids = idx_ref[:, b * blk:(b + 1) * blk]
        ids = (ids // 2 % 2) * 4 + (ids // 4) * 2 + ids % 2
        one_hot = (lax.broadcasted_iota(jnp.int32, (16, blk), 0) == ids).astype(jnp.float32)
        before = jnp.dot(one_hot.astype(jnp.bfloat16), tri, preferred_element_type=jnp.float32) + running
        slot = jnp.sum(one_hot * before, axis=0, keepdims=True)
        running = running + jnp.sum(one_hot, axis=1, keepdims=True)
        row = jnp.where(slot < cap, ids.astype(jnp.float32) * cap + slot, -1.0)
        dest[b:b + 1, :] = row.astype(jnp.int32)
        cols[b, :, 0:1] = jnp.sum(jnp.where(eye, row, 0.0), axis=1, keepdims=True)
        cols[b, :, 1:2] = jnp.sum(jnp.where(eye, gate_ref[:, b * blk:(b + 1) * blk], 0.0), axis=1, keepdims=True)

    @pl.loop(0, n_blk)
    def _(b):
        x_load(b).wait()

    def tok_copy(e, dev):
        return pltpu.make_async_remote_copy(
            src_ref=sendb.at[e], dst_ref=recv.at[me], send_sem=tok_send.at[e], recv_sem=tok_recv.at[me],
            device_id=dev, device_id_type=MESH)

    def moved_copy(e):
        return pltpu.make_async_remote_copy(
            src_ref=sendb.at[e], dst_ref=recv.at[n_src + c], send_sem=tok_send.at[e], recv_sem=tok_recv.at[n_src + c],
            device_id={"rep": 1 - x, "data": inward, "expert": 2 * (1 - y) + 1}, device_id_type=MESH)

    def tok_sent():
        for k in range(1, PEERS):
            peer = plane_id(k % 2, (k // 2) % 2, (c + k // 4) % 2)
            tok_copy(plane_num(*peer), plane_dev(*peer)).wait_send()

    @pl.loop(0, PEERS)
    def _(k):
        kk = k % 4
        peer = plane_id((kk + 1) % 2, ((kk + 1) // 2) % 2, k // 4)
        e = plane_num(*peer)
        slots = lax.broadcasted_iota(jnp.int32, (cap, blk), 0) + e * cap

        def pick(b):
            hot = (slots == dest[pl.ds(b, 1), :]).astype(jnp.float32).astype(jnp.bfloat16)
            return jnp.dot(hot, back[b, 0:blk, :], preferred_element_type=jnp.float32)

        acc[0] = pick(0)

        @pl.loop(1, n_blk - 1)
        def _(b):
            acc[0] += pick(b)

        rows = (acc[0] + pick(n_blk - 1)).astype(jnp.bfloat16)

        @pl.when(e == me)
        def _():
            recv[me] = rows

        @pl.when(e != me)
        def _():
            sendb[e] = rows

            @pl.when(jnp.logical_and(outer, k == 6))
            def _():
                moved_copy(e).start()

            @pl.when(jnp.logical_or(inner, k != 6))
            def _():
                tok_copy(e, plane_dev(*peer)).start()

        def at(step):
            return pl.when(jnp.logical_and(a_inner, k == step))

        @at(1)
        def _():
            light_end(0)
            light_own(3)

        @at(2)
        def _():
            light_end(1)
            light_own(4)
            heavy_mate(0)
            heavy_mate(1)
            heavy_own(3)

        @at(3)
        def _():
            light_end(2)
            light_own(5)

        @at(4)
        def _():
            light_end(3)
            heavy_mate(2)
            heavy_far(0)
            heavy_own(4)

        @at(5)
        def _():
            light_end(4)

        @at(6)
        def _():
            light_end(5)
            heavy_mate(3)
            heavy_far(1)
            heavy_own(5)

        @pl.when(jnp.logical_and(jnp.logical_and(is_a, outer), k == 6))
        def _():
            go(sent_outer, 0)

    for k in range(1, PEERS):
        dev = plane_dev(*plane_id(k % 2, (k // 2) % 2, (c + k // 4) % 2))
        pl.semaphore_signal(ready_sem, inc=1, device_id=dev, device_id_type=MESH)

    @pl.when(outer)
    def _():
        pl.semaphore_signal(ready_sem, inc=1, device_id={"data": inward}, device_id_type=MESH)

    @pl.loop(0, n_src)
    def _(s):
        acc[s] = jnp.zeros((cap, d_model), jnp.float32)

    def tok_arrived(s):
        pltpu.make_async_remote_copy(
            src_ref=sendb.at[0], dst_ref=recv.at[s], send_sem=tok_send.at[0], recv_sem=tok_recv.at[s],
            device_id={"data": inward}, device_id_type=MESH).wait_recv()

    @pl.when(a_inner)
    def _():
        heavy_mate(4)
        heavy_far(2)

    @pl.when(c == 1)
    def _():
        pl.semaphore_wait(go_sem.at[0], 1)

        @pl.when(outer)
        def _():
            own_outer()

        @pl.when(inner)
        def _():
            @pl.loop(0, n_chunk)
            def _(j):
                light_own(j)
                light_end(j)

    for k in range(1, PEERS):
        peer = plane_id(k % 2, (k // 2) % 2, (c + k // 4) % 2)
        s = plane_num(*peer)

        @pl.when(jnp.logical_not(b_outer) if k % 4 == 3 else s >= 0)
        def _():
            tok_arrived(s)

    @pl.when(a_inner)
    def _():
        heavy_mate(5)

    @pl.when(is_b)
    def _():
        tok_sent()

    @pl.when(b_inner)
    def _():
        for owner in (mate, far):
            for m in range(3):
                w_copy(0, owner, m, True, end).wait_recv()

    def ffn(j, s):
        rows = recv[s]
        g = jnp.dot(rows, wg_buf[j], preferred_element_type=jnp.float32)
        u = jnp.dot(rows, wu_buf[j], preferred_element_type=jnp.float32)
        h = (g * jax.nn.sigmoid(g) * u).astype(jnp.bfloat16)
        return lax.dot_general(h, wd_buf[j], (((1,), (1,)), ((), ())), preferred_element_type=jnp.float32)

    def ret_piece(e, q):
        return back.at[e, pl.ds(q * low, cap - low if q else low), :]

    def returned(e, qs):
        @pl.when(e != me)
        def _():
            for q in qs:
                pltpu.make_async_remote_copy(
                    src_ref=ret_piece(e, q), dst_ref=ret_piece(e, q), send_sem=ret_send.at[e, q], recv_sem=ret_recv.at[e, q],
                    device_id={"data": inward}, device_id_type=MESH).wait_recv()

    def put_back(b, target, rows):
        hot = (target.astype(jnp.float32) == cols[b, :, 0:1]).astype(jnp.float32).astype(jnp.bfloat16)
        return jnp.dot(hot, rows.reshape(target.shape[1], d_model), preferred_element_type=jnp.float32)

    def first_half(k):
        e = 2 * ((y + k) % 2)
        for dx in range(2):
            returned(e + dx, (0, 1))
        target = lax.broadcasted_iota(jnp.int32, (1, 2 * cap), 1) + e * cap

        @pl.loop(0, n_blk)
        def _(b):
            got = put_back(b, target, back[pl.ds(e, 2)])
            if k == 1:
                got += sendb[b, 0:blk, :].astype(jnp.float32)
            sendb[b, 0:blk, :] = got.astype(jnp.bfloat16)

    def last_half(q):
        rows = cap - low if q else low
        for e in range(4, 8):
            returned(e, (q,))
        col = lax.broadcasted_iota(jnp.int32, (1, 4 * rows), 1)
        target = (col // rows + 4) * cap + col % rows + q * low
        return target, slice(q * low, q * low + rows)

    def skipped(s):
        return jnp.logical_and(b_outer, s % 4 == 2 * (1 - y) + 1 - x)

    def before_chunk(j):
        @pl.when(outer)
        def _():
            end_wait(j)

    @pl.loop(0, n_chunk - 1)
    def _(j):
        before_chunk(j)

        @pl.loop(0, n_src)
        def _(s):
            @pl.when(jnp.logical_not(skipped(s)))
            def _():
                acc[s] += ffn(j, s)

            @pl.when(jnp.logical_and(b_inner, jnp.logical_and(j == 0, s == 3)))
            def _():
                pl.semaphore_wait(go_sem.at[1], 1)
                for owner in (z, mate, far):
                    pass_on(0, owner, True, False)
                heavy_all(1)

        @pl.when(jnp.logical_and(a_inner, j == 0))
        def _():
            heavy_far(3)
            heavy_far(4)
            go(sent_light, 0)

        @pl.when(jnp.logical_and(a_inner, j == 1))
        def _():
            heavy_far(5)

        @pl.when(jnp.logical_and(a_inner, j == 2))
        def _():
            go(sent_heavy, 1)

        @pl.when(jnp.logical_and(b_inner, j < 4))
        def _():
            heavy_all(j + 2)

        @pl.when(jnp.logical_and(b_outer, j == 2))
        def _():
            first_half(0)

        @pl.when(jnp.logical_and(b_outer, j == 3))
        def _():
            first_half(1)

    def relay_copy(i):
        return pltpu.make_async_remote_copy(
            src_ref=recv.at[n_src + i], dst_ref=relay_hbm, send_sem=relay_send.at[i], recv_sem=relay_recv,
            device_id=plane_dev(1 - x, 1 - y, i), device_id_type=MESH)

    @pl.when(b_inner)
    def _():
        @pl.loop(0, 2)
        def _(i):
            tok_arrived(n_src + i)
            acc[n_src] = ffn(0, n_src + i)

            @pl.loop(1, n_chunk)
            def _(j):
                acc[n_src] += ffn(j, n_src + i)

            recv[n_src + i] = acc[n_src].astype(jnp.bfloat16)
            relay_copy(i).start()

    before_chunk(n_chunk - 1)

    @pl.when(is_a)
    def _():
        tok_sent()

    @pl.when(outer)
    def _():
        pl.semaphore_wait(ready_sem, PEERS - 1)

    @pl.when(inner)
    def _():
        pl.semaphore_wait(ready_sem, PEERS)

    def ret_copy(s, q, dev):
        piece = pl.ds(q * low, cap - low if q else low)
        return pltpu.make_async_remote_copy(
            src_ref=recv.at[s, piece, :], dst_ref=back.at[me, piece, :], send_sem=ret_send.at[s, q], recv_sem=ret_recv.at[me, q],
            device_id=dev, device_id_type=MESH)

    def ret_peer(r):
        q, rr = r // 4, r % 4
        return plane_id((1 - q) * ((rr + 1) % 2) + q * (1 - rr // 2), (1 - q) * (rr % 2) + q * (1 - rr // 2), (c + rr // 2 + q * rr) % 2)

    def ret_needed(s):
        return jnp.logical_and(s != me, jnp.logical_not(skipped(s)))

    @pl.loop(0, PEERS)
    def _(r):
        peer = ret_peer(r)
        s = plane_num(*peer)

        @pl.when(jnp.logical_not(skipped(s)))
        def _():
            rows = (acc[s] + ffn(n_chunk - 1, s)).astype(jnp.bfloat16)

            @pl.when(s == me)
            def _():
                back[me] = rows

            @pl.when(s != me)
            def _():
                recv[s] = rows
                ret_copy(s, 0, plane_dev(*peer)).start()

    @pl.loop(0, PEERS)
    def _(r):
        peer = ret_peer(r)
        s = plane_num(*peer)

        @pl.when(ret_needed(s))
        def _():
            ret_copy(s, 1, plane_dev(*peer)).start()

    @pl.when(jnp.logical_not(b_outer))
    def _():
        first_half(0)
        first_half(1)

    for h in range(2):
        x_again(0, h).start()

    target, piece = last_half(0)

    @pl.loop(0, n_blk)
    def _(b):
        got = put_back(b, target, back[4:8, piece, :]) + sendb[b, 0:blk, :].astype(jnp.float32)
        sendb[b, 0:blk, :] = got.astype(jnp.bfloat16)

    def fwd_copy(q):
        piece = pl.ds(q * low, cap - low if q else low)
        e = 4 + 2 * (1 - y) + 1 - x
        return pltpu.make_async_remote_copy(
            src_ref=relay_hbm.at[piece, :], dst_ref=back.at[e, piece, :], send_sem=fwd_send.at[q], recv_sem=ret_recv.at[e, q],
            device_id={"data": end}, device_id_type=MESH)

    @pl.when(inner)
    def _():
        pltpu.make_async_remote_copy(
            src_ref=recv.at[0], dst_ref=relay_hbm, send_sem=relay_send.at[0], recv_sem=relay_recv,
            device_id={"data": mate}, device_id_type=MESH).wait_recv()

        @pl.when(is_b)
        def _():
            @pl.loop(0, n_chunk)
            def _(j):
                sent_heavy(j)

            pl.semaphore_signal(go_sem.at[2], inc=1, device_id={"expert": p - 1}, device_id_type=MESH)

        @pl.when(is_a)
        def _():
            pl.semaphore_wait(go_sem.at[2], 1)

        for q in range(2):
            fwd_copy(q).start()

    target_hi, piece_hi = last_half(1)

    def out_copy(b):
        return pltpu.make_async_copy(sendb.at[b, pl.ds(0, blk), :], x_rows(out_hbm, b), out_sem.at[b])

    @pl.loop(0, n_blk)
    def _(b):
        mixed = (put_back(b, target_hi, back[4:8, piece_hi, :]) + sendb[b, 0:blk, :].astype(jnp.float32)) * cols[b, :, 1:2]
        for h in range(2):
            part = slice(h * half, h * half + half)
            x_again(b, h).wait()
            sendb[b, part, :] = (x_buf[h].astype(jnp.float32) + mixed[part]).astype(jnp.bfloat16)

            @pl.when(b + 1 < n_blk)
            def _():
                x_again(b + 1, h).start()

        out_copy(b).start()

    @pl.loop((n_chunk - 1) * (1 - c), n_chunk)
    def _(j):
        @pl.when(outer)
        def _():
            sent_outer(j)

        @pl.when(inner)
        def _():
            sent_light(j)

    @pl.when(a_inner)
    def _():
        sent_heavy(n_chunk - 1)

    @pl.when(b_inner)
    def _():
        for i in range(2):
            relay_copy(i).wait_send()

    @pl.when(inner)
    def _():
        for q in range(2):
            fwd_copy(q).wait_send()

    @pl.loop(0, PEERS)
    def _(r):
        peer = ret_peer(r)
        s = plane_num(*peer)

        @pl.when(ret_needed(s))
        def _():
            for q in range(2):
                ret_copy(s, q, plane_dev(*peer)).wait_send()

    @pl.loop(0, n_blk)
    def _(b):
        out_copy(b).wait()


def solution(mesh):
    n_group = mesh.shape["expert"]
    tok_spec = P(("rep", "expert", "data"), None)
    wide_spec = P("expert", "data", None)
    down_spec = P("expert", None, "data")

    def device_step(x_loc, idx_loc, gate_loc, wg_loc, wu_loc, wd_loc):
        tok_rows, d_model = x_loc.shape
        top_k = idx_loc.shape[1]
        n_exp = wg_loc.shape[0] * n_group
        ffn = wg_loc.shape[2]
        cap = capacity_rows(tok_rows, top_k, n_exp)
        blk = tok_rows // PEERS
        f_chunk = ffn // CHUNKS
        any_spec = pl.BlockSpec(memory_space=pl.ANY)
        vmem_spec = pl.BlockSpec(memory_space=pltpu.VMEM)
        dma = pltpu.SemaphoreType.DMA
        return pl.pallas_call(
            moe_kernel,
            out_shape=(jax.ShapeDtypeStruct((tok_rows, d_model), jnp.bfloat16), jax.ShapeDtypeStruct((cap, d_model), jnp.bfloat16)),
            in_specs=[any_spec, vmem_spec, vmem_spec, any_spec, any_spec, any_spec],
            out_specs=(any_spec, any_spec),
            scratch_shapes=[
                pltpu.VMEM((CHUNKS, d_model, f_chunk), jnp.bfloat16),
                pltpu.VMEM((CHUNKS, d_model, f_chunk), jnp.bfloat16),
                pltpu.VMEM((CHUNKS, d_model, f_chunk), jnp.bfloat16),
                pltpu.VMEM((PEERS + 2, cap, d_model), jnp.bfloat16),
                pltpu.VMEM((PEERS, cap, d_model), jnp.bfloat16),
                pltpu.VMEM((PEERS, cap, d_model), jnp.bfloat16),
                pltpu.VMEM((PEERS + 1, cap, d_model), jnp.float32),
                pltpu.VMEM((2, blk // 2, d_model), jnp.bfloat16),
                pltpu.VMEM((PEERS, blk), jnp.int32),
                pltpu.VMEM((PEERS, blk, 2), jnp.float32),
                dma((CHUNKS, NZ, 3)), dma((CHUNKS, NZ, 3)), dma((CHUNKS, NZ, 3)),
                dma((PEERS + 2,)), dma((PEERS,)), dma((PEERS, 2)), dma((PEERS, 2)), dma, dma((2,)), dma((2,)),
                dma((PEERS,)), dma((PEERS,)), pltpu.SemaphoreType.REGULAR((3,)), pltpu.SemaphoreType.REGULAR,
            ],
            compiler_params=pltpu.CompilerParams(collective_id=0, has_side_effects=True, vmem_limit_bytes=VMEM_BYTES),
        )(x_loc, idx_loc.T, gate_loc.T, wg_loc, wu_loc, wd_loc.transpose(0, 2, 1))[0]

    return jax.shard_map(device_step, mesh=mesh, in_specs=(tok_spec, tok_spec, tok_spec, wide_spec, wide_spec, down_spec), out_specs=tok_spec, check_vma=False)
```

```python
import functools

import jax
import jax.numpy as jnp
from jax import lax
from jax.experimental import pallas as pl
from jax.experimental.pallas import tpu as pltpu
from jax.sharding import PartitionSpec as P

MESH = pl.DeviceIdType.MESH
CHUNKS = 6
NZ = 4
PEERS = 8
AHEAD = 3
VMEM_BYTES = 67_000_000


def capacity_rows(tok_rows, top_k, n_exp):
    return max(8, ((5 * top_k * tok_rows) // (4 * n_exp) + 7) // 8 * 8)


def low_rows(cap):
    return cap * 3 // 5 // 8 * 8


def moe_kernel(x_hbm, idx_ref, gate_ref, wg_hbm, wu_hbm, wd_hbm, out_hbm, relay_hbm,
               wg_buf, wu_buf, wd_buf, recv, sendb, back, acc, x_buf, dest, cols,
               w_recv, w_light, w_heavy, tok_recv, tok_send, ret_recv, ret_send, relay_recv, relay_send, fwd_send,
               x_sem, out_sem, go_sem, ready_sem):
    n_src, cap, d_model = back.shape
    low = low_rows(cap)
    n_blk, blk, _ = cols.shape
    n_chunk, _, f_chunk = wg_buf.shape
    shard = d_model // NZ

    x = lax.axis_index("rep")
    z = lax.axis_index("data")
    p = lax.axis_index("expert")
    y, c = p // 2, p % 2
    me = 4 * c + 2 * y + x
    is_a = c == 0
    inner = jnp.logical_and(z > 0, z < NZ - 1)
    outer = jnp.logical_or(z == 0, z == NZ - 1)
    is_b = c == 1
    a_inner = jnp.logical_and(is_a, inner)
    b_inner = jnp.logical_and(is_b, inner)
    b_outer = jnp.logical_and(is_b, outer)
    inward = (z + 3) // 3

    def plane_id(dx, dy, cc):
        return (x + dx) % 2, (y + dy) % 2, cc

    def plane_dev(px, py, pc):
        return {"rep": px, "expert": 2 * py + pc}

    def plane_num(px, py, pc):
        return 4 * pc + 2 * py + px

    def w_view(j, s, m):
        return (wg_buf, wu_buf, wd_buf)[m].at[j, pl.ds(s * shard, shard), :]

    def w_local(j, m):
        src = (wg_hbm, wu_hbm, wd_hbm)[m].at[x, :, pl.ds(pl.multiple_of(j * f_chunk, f_chunk), f_chunk)]
        return pltpu.make_async_copy(src, w_view(j, z, m), w_recv.at[j, z, m])

    def w_copy(j, s, m, heavy, dev):
        view = w_view(j, s, m)
        return pltpu.make_async_remote_copy(
            src_ref=view, dst_ref=view, send_sem=(w_heavy if heavy else w_light).at[j, s, m], recv_sem=w_recv.at[j, s, m],
            device_id={"data": dev}, device_id_type=MESH)

    end, far, mate = 3 * (z - 1), 3 * (2 - z), 3 - z

    def pass_on(j, s, heavy, arrives=True):
        for m in range(3):
            cp = w_copy(j, s, m, heavy, end if heavy else mate)
            if arrives:
                cp.wait_recv()
            cp.start()

    def light_own(j):
        pass_on(j, z, False, False)

    def light_end(j):
        pass_on(j, end, False)

    def heavy_own(j):
        pass_on(j, z, True, False)

    def heavy_mate(j):
        pass_on(j, mate, True)

    def heavy_far(j):
        pass_on(j, far, True)

    def heavy_all(j):
        heavy_own(j)
        heavy_mate(j)
        heavy_far(j)

    def own_outer():
        @pl.loop(0, n_chunk)
        def _(j):
            for m in range(3):
                w_copy(j, z, m, False, inward).start()

    def end_wait(j):
        for d in range(1, NZ):
            for m in range(3):
                w_copy(j, (z + d) % NZ, m, False, inward).wait_recv()

    def sent(j, shards, heavy):
        for s in shards:
            for m in range(3):
                w_copy(j, s, m, heavy, (z + 1) % NZ).wait_send()

    def sent_outer(j):
        sent(j, (z,), False)

    def sent_light(j):
        sent(j, (z, end), False)

    def sent_heavy(j):
        sent(j, (z, mate, far), True)

    def go(done, heavy):
        @pl.loop(0, n_chunk - 1)
        def _(j):
            done(j)

        pl.semaphore_signal(go_sem.at[heavy], inc=1, device_id={"expert": p + 1}, device_id_type=MESH)

    def x_rows(ref, b):
        return ref.at[pl.ds(pl.multiple_of(b * blk, blk), blk), :]

    def x_load(b):
        return pltpu.make_async_copy(x_rows(x_hbm, b), back.at[b, pl.ds(0, blk), :], x_sem.at[b])

    half = blk // 2

    def x_again(b, h):
        rows = pl.ds(pl.multiple_of(b * blk + h * half, half), half)
        return pltpu.make_async_copy(x_hbm.at[rows, :], x_buf.at[h], x_sem.at[h])

    @pl.loop(0, n_chunk)
    def _(j):
        for m in range(3):
            w_local(j, m).start()

    @pl.loop(0, n_blk)
    def _(b):
        x_load(b).start()

    barrier = pltpu.get_barrier_semaphore()
    for k in range(1, PEERS):
        dev = plane_dev(*plane_id(k % 2, (k // 2) % 2, (c + k // 4) % 2))
        pl.semaphore_signal(barrier, inc=1, device_id=dev, device_id_type=MESH)

    @pl.when(z > 0)
    def _():
        pl.semaphore_signal(barrier, inc=1, device_id={"data": z - 1}, device_id_type=MESH)

    @pl.when(z < NZ - 1)
    def _():
        pl.semaphore_signal(barrier, inc=1, device_id={"data": z + 1}, device_id_type=MESH)

    @pl.when(outer)
    def _():
        pl.semaphore_wait(barrier, PEERS)

    @pl.when(inner)
    def _():
        pl.semaphore_wait(barrier, PEERS + 1)

    @pl.loop(0, n_chunk)
    def _(j):
        for m in range(3):
            w_local(j, m).wait()

    @pl.when(is_a)
    def _():
        @pl.when(outer)
        def _():
            own_outer()

        @pl.when(inner)
        def _():
            for j in range(AHEAD):
                light_own(j)
                heavy_own(j)

    tri = (lax.broadcasted_iota(jnp.int32, (blk, blk), 0) < lax.broadcasted_iota(jnp.int32, (blk, blk), 1)).astype(jnp.float32).astype(jnp.bfloat16)
    eye = lax.broadcasted_iota(jnp.int32, (blk, blk), 0) == lax.broadcasted_iota(jnp.int32, (blk, blk), 1)
    running = jnp.zeros((16, 1), jnp.float32)
    for b in range(n_blk):
        ids = idx_ref[:, b * blk:(b + 1) * blk]
        ids = (ids // 2 % 2) * 4 + (ids // 4) * 2 + ids % 2
        one_hot = (lax.broadcasted_iota(jnp.int32, (16, blk), 0) == ids).astype(jnp.float32)
        before = jnp.dot(one_hot.astype(jnp.bfloat16), tri, preferred_element_type=jnp.float32) + running
        slot = jnp.sum(one_hot * before, axis=0, keepdims=True)
        running = running + jnp.sum(one_hot, axis=1, keepdims=True)
        row = jnp.where(slot < cap, ids.astype(jnp.float32) * cap + slot, -1.0)
        dest[b:b + 1, :] = row.astype(jnp.int32)
        cols[b, :, 0:1] = jnp.sum(jnp.where(eye, row, 0.0), axis=1, keepdims=True)
        cols[b, :, 1:2] = jnp.sum(jnp.where(eye, gate_ref[:, b * blk:(b + 1) * blk], 0.0), axis=1, keepdims=True)

    @pl.loop(0, n_blk)
    def _(b):
        x_load(b).wait()

    def tok_copy(e, dev):
        return pltpu.make_async_remote_copy(
            src_ref=sendb.at[e], dst_ref=recv.at[me], send_sem=tok_send.at[e], recv_sem=tok_recv.at[me],
            device_id=dev, device_id_type=MESH)

    def tok_sent():
        for k in range(1, PEERS):
            peer = plane_id(k % 2, (k // 2) % 2, (c + k // 4) % 2)
            tok_copy(plane_num(*peer), plane_dev(*peer)).wait_send()

    @pl.loop(0, PEERS)
    def _(k):
        kk = k % 4
        peer = plane_id((kk + 1) % 2, ((kk + 1) // 2) % 2, k // 4)
        e = plane_num(*peer)
        slots = lax.broadcasted_iota(jnp.int32, (cap, blk), 0) + e * cap

        def pick(b):
            hot = (slots == dest[pl.ds(b, 1), :]).astype(jnp.float32).astype(jnp.bfloat16)
            return jnp.dot(hot, back[b, 0:blk, :], preferred_element_type=jnp.float32)

        acc[0] = pick(0)

        @pl.loop(1, n_blk - 1)
        def _(b):
            acc[0] += pick(b)

        rows = (acc[0] + pick(n_blk - 1)).astype(jnp.bfloat16)

        @pl.when(e == me)
        def _():
            recv[me] = rows

        @pl.when(e != me)
        def _():
            sendb[e] = rows

            tok_copy(e, plane_dev(*peer)).start()

        def at(step):
            return pl.when(jnp.logical_and(a_inner, k == step))

        @at(1)
        def _():
            light_end(0)
            light_own(3)

        @at(2)
        def _():
            light_end(1)
            light_own(4)
            heavy_mate(0)
            heavy_mate(1)
            heavy_own(3)

        @at(3)
        def _():
            light_end(2)
            light_own(5)

        @at(4)
        def _():
            light_end(3)
            heavy_mate(2)
            heavy_far(0)
            heavy_own(4)

        @at(5)
        def _():
            light_end(4)

        @at(6)
        def _():
            light_end(5)
            heavy_mate(3)
            heavy_far(1)
            heavy_own(5)

        @pl.when(jnp.logical_and(jnp.logical_and(is_a, outer), k == 6))
        def _():
            go(sent_outer, 0)

    for k in range(1, PEERS):
        dev = plane_dev(*plane_id(k % 2, (k // 2) % 2, (c + k // 4) % 2))
        pl.semaphore_signal(ready_sem, inc=1, device_id=dev, device_id_type=MESH)

    @pl.when(outer)
    def _():
        pl.semaphore_signal(ready_sem, inc=1, device_id={"data": inward}, device_id_type=MESH)

    @pl.loop(0, n_src)
    def _(s):
        acc[s] = jnp.zeros((cap, d_model), jnp.float32)

    def tok_arrived(s):
        pltpu.make_async_remote_copy(
            src_ref=sendb.at[0], dst_ref=recv.at[s], send_sem=tok_send.at[0], recv_sem=tok_recv.at[s],
            device_id={"data": inward}, device_id_type=MESH).wait_recv()

    @pl.when(a_inner)
    def _():
        heavy_mate(4)
        heavy_far(2)

    @pl.when(c == 1)
    def _():
        pl.semaphore_wait(go_sem.at[0], 1)

        @pl.when(outer)
        def _():
            own_outer()

        @pl.when(inner)
        def _():
            @pl.loop(0, n_chunk)
            def _(j):
                light_own(j)
                light_end(j)

    for k in range(1, PEERS):
        peer = plane_id(k % 2, (k // 2) % 2, (c + k // 4) % 2)
        s = plane_num(*peer)
        tok_arrived(s)

    def moved_copy(i):
        return pltpu.make_async_remote_copy(
            src_ref=recv.at[plane_num(1 - x, 1 - y, i)], dst_ref=recv.at[n_src + i], send_sem=relay_send.at[i],
            recv_sem=tok_recv.at[n_src + i], device_id={"data": inward}, device_id_type=MESH)

    @pl.when(b_outer)
    def _():
        for i in range(2):
            moved_copy(i).start()

    @pl.when(a_inner)
    def _():
        heavy_mate(5)

    @pl.when(is_b)
    def _():
        tok_sent()

    @pl.when(b_inner)
    def _():
        for owner in (mate, far):
            for m in range(3):
                w_copy(0, owner, m, True, end).wait_recv()

    def ffn(j, s):
        rows = recv[s]
        g = jnp.dot(rows, wg_buf[j], preferred_element_type=jnp.float32)
        u = jnp.dot(rows, wu_buf[j], preferred_element_type=jnp.float32)
        h = (g * jax.nn.sigmoid(g) * u).astype(jnp.bfloat16)
        return lax.dot_general(h, wd_buf[j], (((1,), (1,)), ((), ())), preferred_element_type=jnp.float32)

    def ret_piece(e, q):
        return back.at[e, pl.ds(q * low, cap - low if q else low), :]

    def returned(e, qs):
        @pl.when(e != me)
        def _():
            for q in qs:
                pltpu.make_async_remote_copy(
                    src_ref=ret_piece(e, q), dst_ref=ret_piece(e, q), send_sem=ret_send.at[e, q], recv_sem=ret_recv.at[e, q],
                    device_id={"data": inward}, device_id_type=MESH).wait_recv()

    def put_back(b, target, rows):
        hot = (target.astype(jnp.float32) == cols[b, :, 0:1]).astype(jnp.float32).astype(jnp.bfloat16)
        return jnp.dot(hot, rows.reshape(target.shape[1], d_model), preferred_element_type=jnp.float32)

    def first_half(k):
        e = 2 * ((y + k) % 2)
        for dx in range(2):
            returned(e + dx, (0, 1))
        target = lax.broadcasted_iota(jnp.int32, (1, 2 * cap), 1) + e * cap

        @pl.loop(0, n_blk)
        def _(b):
            got = put_back(b, target, back[pl.ds(e, 2)])
            if k == 1:
                got += sendb[b, 0:blk, :].astype(jnp.float32)
            sendb[b, 0:blk, :] = got.astype(jnp.bfloat16)

    def last_half(q):
        rows = cap - low if q else low
        for e in range(4, 8):
            returned(e, (q,))
        col = lax.broadcasted_iota(jnp.int32, (1, 4 * rows), 1)
        target = (col // rows + 4) * cap + col % rows + q * low
        return target, slice(q * low, q * low + rows)

    def skipped(s):
        return jnp.logical_and(b_outer, s % 4 == 2 * (1 - y) + 1 - x)

    def before_chunk(j):
        @pl.when(outer)
        def _():
            end_wait(j)

    @pl.loop(0, n_chunk - 1)
    def _(j):
        before_chunk(j)

        @pl.loop(0, n_src)
        def _(s):
            @pl.when(jnp.logical_not(skipped(s)))
            def _():
                acc[s] += ffn(j, s)

            @pl.when(jnp.logical_and(b_inner, jnp.logical_and(j == 0, s == 3)))
            def _():
                pl.semaphore_wait(go_sem.at[1], 1)
                for owner in (z, mate, far):
                    pass_on(0, owner, True, False)
                heavy_all(1)

        @pl.when(jnp.logical_and(a_inner, j == 0))
        def _():
            heavy_far(3)
            heavy_far(4)
            go(sent_light, 0)

        @pl.when(jnp.logical_and(a_inner, j == 1))
        def _():
            heavy_far(5)

        @pl.when(jnp.logical_and(a_inner, j == 2))
        def _():
            go(sent_heavy, 1)

        @pl.when(jnp.logical_and(b_inner, j < 4))
        def _():
            heavy_all(j + 2)

        @pl.when(jnp.logical_and(b_outer, j == 2))
        def _():
            first_half(0)

        @pl.when(jnp.logical_and(b_outer, j == 3))
        def _():
            first_half(1)

    def relay_copy(i):
        return pltpu.make_async_remote_copy(
            src_ref=recv.at[n_src + i], dst_ref=relay_hbm, send_sem=relay_send.at[i], recv_sem=relay_recv,
            device_id=plane_dev(1 - x, 1 - y, i), device_id_type=MESH)

    @pl.when(b_inner)
    def _():
        @pl.loop(0, 2)
        def _(i):
            tok_arrived(n_src + i)
            acc[n_src] = ffn(0, n_src + i)

            @pl.loop(1, n_chunk)
            def _(j):
                acc[n_src] += ffn(j, n_src + i)

            recv[n_src + i] = acc[n_src].astype(jnp.bfloat16)
            relay_copy(i).start()

    before_chunk(n_chunk - 1)

    @pl.when(is_a)
    def _():
        tok_sent()

    @pl.when(outer)
    def _():
        pl.semaphore_wait(ready_sem, PEERS - 1)

    @pl.when(inner)
    def _():
        pl.semaphore_wait(ready_sem, PEERS)

    def ret_copy(s, q, dev):
        piece = pl.ds(q * low, cap - low if q else low)
        return pltpu.make_async_remote_copy(
            src_ref=recv.at[s, piece, :], dst_ref=back.at[me, piece, :], send_sem=ret_send.at[s, q], recv_sem=ret_recv.at[me, q],
            device_id=dev, device_id_type=MESH)

    def ret_peer(r):
        q, rr = r // 4, r % 4
        return plane_id((1 - q) * ((rr + 1) % 2) + q * (1 - rr // 2), (1 - q) * (rr % 2) + q * (1 - rr // 2), (c + rr // 2 + q * rr) % 2)

    def ret_needed(s):
        return jnp.logical_and(s != me, jnp.logical_not(skipped(s)))

    @pl.loop(0, PEERS)
    def _(r):
        peer = ret_peer(r)
        s = plane_num(*peer)

        @pl.when(jnp.logical_not(skipped(s)))
        def _():
            rows = (acc[s] + ffn(n_chunk - 1, s)).astype(jnp.bfloat16)

            @pl.when(s == me)
            def _():
                back[me] = rows

            @pl.when(s != me)
            def _():
                recv[s] = rows
                ret_copy(s, 0, plane_dev(*peer)).start()

    @pl.loop(0, PEERS)
    def _(r):
        peer = ret_peer(r)
        s = plane_num(*peer)

        @pl.when(ret_needed(s))
        def _():
            ret_copy(s, 1, plane_dev(*peer)).start()

    def fwd_copy(q):
        piece = pl.ds(q * low, cap - low if q else low)
        e = 4 + 2 * (1 - y) + 1 - x
        return pltpu.make_async_remote_copy(
            src_ref=relay_hbm.at[piece, :], dst_ref=back.at[e, piece, :], send_sem=fwd_send.at[q], recv_sem=ret_recv.at[e, q],
            device_id={"data": end}, device_id_type=MESH)

    def relay():
        pltpu.make_async_remote_copy(
            src_ref=recv.at[0], dst_ref=relay_hbm, send_sem=relay_send.at[0], recv_sem=relay_recv,
            device_id={"data": mate}, device_id_type=MESH).wait_recv()

        @pl.when(is_b)
        def _():
            @pl.loop(0, n_chunk)
            def _(j):
                sent_heavy(j)

            pl.semaphore_signal(go_sem.at[2], inc=1, device_id={"expert": p - 1}, device_id_type=MESH)

        @pl.when(is_a)
        def _():
            pl.semaphore_wait(go_sem.at[2], 1)

        for q in range(2):
            fwd_copy(q).start()

    @pl.when(jnp.logical_not(b_outer))
    def _():
        first_half(0)

        @pl.when(b_inner)
        def _():
            relay()

        first_half(1)

        @pl.when(a_inner)
        def _():
            relay()

    for h in range(2):
        x_again(0, h).start()

    target, piece = last_half(0)

    @pl.loop(0, n_blk)
    def _(b):
        got = put_back(b, target, back[4:8, piece, :]) + sendb[b, 0:blk, :].astype(jnp.float32)
        sendb[b, 0:blk, :] = got.astype(jnp.bfloat16)

    target_hi, piece_hi = last_half(1)

    def out_copy(b):
        return pltpu.make_async_copy(sendb.at[b, pl.ds(0, blk), :], x_rows(out_hbm, b), out_sem.at[b])

    @pl.loop(0, n_blk)
    def _(b):
        mixed = (put_back(b, target_hi, back[4:8, piece_hi, :]) + sendb[b, 0:blk, :].astype(jnp.float32)) * cols[b, :, 1:2]
        for h in range(2):
            part = slice(h * half, h * half + half)
            x_again(b, h).wait()
            sendb[b, part, :] = (x_buf[h].astype(jnp.float32) + mixed[part]).astype(jnp.bfloat16)

            @pl.when(b + 1 < n_blk)
            def _():
                x_again(b + 1, h).start()

        out_copy(b).start()

    @pl.loop((n_chunk - 1) * (1 - c), n_chunk)
    def _(j):
        @pl.when(outer)
        def _():
            sent_outer(j)

        @pl.when(inner)
        def _():
            sent_light(j)

    @pl.when(a_inner)
    def _():
        sent_heavy(n_chunk - 1)

    @pl.when(b_inner)
    def _():
        for i in range(2):
            relay_copy(i).wait_send()

    @pl.when(b_outer)
    def _():
        for i in range(2):
            moved_copy(i).wait_send()

    @pl.when(inner)
    def _():
        for q in range(2):
            fwd_copy(q).wait_send()

    @pl.loop(0, PEERS)
    def _(r):
        peer = ret_peer(r)
        s = plane_num(*peer)

        @pl.when(ret_needed(s))
        def _():
            for q in range(2):
                ret_copy(s, q, plane_dev(*peer)).wait_send()

    @pl.loop(0, n_blk)
    def _(b):
        out_copy(b).wait()


def solution(mesh):
    n_group = mesh.shape["expert"]
    tok_spec = P(("rep", "expert", "data"), None)
    wide_spec = P("expert", "data", None)
    down_spec = P("expert", None, "data")

    def device_step(x_loc, idx_loc, gate_loc, wg_loc, wu_loc, wd_loc):
        tok_rows, d_model = x_loc.shape
        top_k = idx_loc.shape[1]
        n_exp = wg_loc.shape[0] * n_group
        ffn = wg_loc.shape[2]
        cap = capacity_rows(tok_rows, top_k, n_exp)
        blk = tok_rows // PEERS
        f_chunk = ffn // CHUNKS
        any_spec = pl.BlockSpec(memory_space=pl.ANY)
        vmem_spec = pl.BlockSpec(memory_space=pltpu.VMEM)
        dma = pltpu.SemaphoreType.DMA
        return pl.pallas_call(
            moe_kernel,
            out_shape=(jax.ShapeDtypeStruct((tok_rows, d_model), jnp.bfloat16), jax.ShapeDtypeStruct((cap, d_model), jnp.bfloat16)),
            in_specs=[any_spec, vmem_spec, vmem_spec, any_spec, any_spec, any_spec],
            out_specs=(any_spec, any_spec),
            scratch_shapes=[
                pltpu.VMEM((CHUNKS, d_model, f_chunk), jnp.bfloat16),
                pltpu.VMEM((CHUNKS, d_model, f_chunk), jnp.bfloat16),
                pltpu.VMEM((CHUNKS, d_model, f_chunk), jnp.bfloat16),
                pltpu.VMEM((PEERS + 2, cap, d_model), jnp.bfloat16),
                pltpu.VMEM((PEERS, cap, d_model), jnp.bfloat16),
                pltpu.VMEM((PEERS, cap, d_model), jnp.bfloat16),
                pltpu.VMEM((PEERS + 1, cap, d_model), jnp.float32),
                pltpu.VMEM((2, blk // 2, d_model), jnp.bfloat16),
                pltpu.VMEM((PEERS, blk), jnp.int32),
                pltpu.VMEM((PEERS, blk, 2), jnp.float32),
                dma((CHUNKS, NZ, 3)), dma((CHUNKS, NZ, 3)), dma((CHUNKS, NZ, 3)),
                dma((PEERS + 2,)), dma((PEERS,)), dma((PEERS, 2)), dma((PEERS, 2)), dma, dma((2,)), dma((2,)),
                dma((PEERS,)), dma((PEERS,)), pltpu.SemaphoreType.REGULAR((3,)), pltpu.SemaphoreType.REGULAR,
            ],
            compiler_params=pltpu.CompilerParams(collective_id=0, has_side_effects=True, vmem_limit_bytes=VMEM_BYTES),
        )(x_loc, idx_loc.T, gate_loc.T, wg_loc, wu_loc, wd_loc.transpose(0, 2, 1))[0]

    return jax.shard_map(device_step, mesh=mesh, in_specs=(tok_spec, tok_spec, tok_spec, wide_spec, wide_spec, down_spec), out_specs=tok_spec, check_vma=False)
```

```python
import functools

import jax
import jax.numpy as jnp
from jax import lax
from jax.experimental import pallas as pl
from jax.experimental.pallas import tpu as pltpu
from jax.sharding import PartitionSpec as P

MESH = pl.DeviceIdType.MESH
CHUNKS = 6
NZ = 4
PEERS = 8
AHEAD = 3
VMEM_BYTES = 67_000_000


def capacity_rows(tok_rows, top_k, n_exp):
    return max(8, ((5 * top_k * tok_rows) // (4 * n_exp) + 7) // 8 * 8)


def slot_edges(cap):
    return 0, cap * 2 // 5, cap * 4 // 5, cap


def moe_kernel(x_hbm, idx_ref, gate_ref, wg_hbm, wu_hbm, wd_hbm, out_hbm, relay_hbm,
               wg_buf, wu_buf, wd_buf, recv, sendb, back, acc, x_buf, dest, cols,
               w_recv, w_light, w_heavy, tok_recv, tok_send, ret_recv, ret_send, relay_recv, relay_send, fwd_send,
               x_sem, out_sem, go_sem, ready_sem):
    n_src, cap, d_model = back.shape
    edges = slot_edges(cap)
    pieces = range(len(edges) - 1)
    n_blk, blk, _ = cols.shape
    n_chunk, _, f_chunk = wg_buf.shape
    shard = d_model // NZ

    x = lax.axis_index("rep")
    z = lax.axis_index("data")
    p = lax.axis_index("expert")
    y, c = p // 2, p % 2
    me = 4 * c + 2 * y + x
    is_a = c == 0
    inner = jnp.logical_and(z > 0, z < NZ - 1)
    outer = jnp.logical_or(z == 0, z == NZ - 1)
    is_b = c == 1
    a_inner = jnp.logical_and(is_a, inner)
    b_inner = jnp.logical_and(is_b, inner)
    b_outer = jnp.logical_and(is_b, outer)
    inward = (z + 3) // 3

    def plane_id(dx, dy, cc):
        return (x + dx) % 2, (y + dy) % 2, cc

    def plane_dev(px, py, pc):
        return {"rep": px, "expert": 2 * py + pc}

    def plane_num(px, py, pc):
        return 4 * pc + 2 * py + px

    def w_view(j, s, m):
        return (wg_buf, wu_buf, wd_buf)[m].at[j, pl.ds(s * shard, shard), :]

    def w_local(j, m):
        src = (wg_hbm, wu_hbm, wd_hbm)[m].at[x, :, pl.ds(pl.multiple_of(j * f_chunk, f_chunk), f_chunk)]
        return pltpu.make_async_copy(src, w_view(j, z, m), w_recv.at[j, z, m])

    def w_copy(j, s, m, heavy, dev):
        view = w_view(j, s, m)
        return pltpu.make_async_remote_copy(
            src_ref=view, dst_ref=view, send_sem=(w_heavy if heavy else w_light).at[j, s, m], recv_sem=w_recv.at[j, s, m],
            device_id={"data": dev}, device_id_type=MESH)

    end, far, mate = 3 * (z - 1), 3 * (2 - z), 3 - z

    def pass_on(j, s, heavy, arrives=True):
        for m in range(3):
            cp = w_copy(j, s, m, heavy, end if heavy else mate)
            if arrives:
                cp.wait_recv()
            cp.start()

    def light_own(j):
        pass_on(j, z, False, False)

    def light_end(j):
        pass_on(j, end, False)

    def heavy_own(j):
        pass_on(j, z, True, False)

    def heavy_mate(j):
        pass_on(j, mate, True)

    def heavy_far(j):
        pass_on(j, far, True)

    def heavy_all(j):
        heavy_own(j)
        heavy_mate(j)
        heavy_far(j)

    def own_outer():
        @pl.loop(0, n_chunk)
        def _(j):
            for m in range(3):
                w_copy(j, z, m, False, inward).start()

    def end_wait(j):
        for d in range(1, NZ):
            for m in range(3):
                w_copy(j, (z + d) % NZ, m, False, inward).wait_recv()

    def sent(j, shards, heavy):
        for s in shards:
            for m in range(3):
                w_copy(j, s, m, heavy, (z + 1) % NZ).wait_send()

    def sent_outer(j):
        sent(j, (z,), False)

    def sent_light(j):
        sent(j, (z, end), False)

    def sent_heavy(j):
        sent(j, (z, mate, far), True)

    def go(done, heavy):
        @pl.loop(0, n_chunk - 1)
        def _(j):
            done(j)

        pl.semaphore_signal(go_sem.at[heavy], inc=1, device_id={"expert": p + 1}, device_id_type=MESH)

    def x_rows(ref, b):
        return ref.at[pl.ds(pl.multiple_of(b * blk, blk), blk), :]

    def x_load(b):
        return pltpu.make_async_copy(x_rows(x_hbm, b), back.at[b, pl.ds(0, blk), :], x_sem.at[b])

    half = blk // 2

    def x_again(b, h):
        rows = pl.ds(pl.multiple_of(b * blk + h * half, half), half)
        return pltpu.make_async_copy(x_hbm.at[rows, :], x_buf.at[h], x_sem.at[h])

    @pl.loop(0, n_chunk)
    def _(j):
        for m in range(3):
            w_local(j, m).start()

    @pl.loop(0, n_blk)
    def _(b):
        x_load(b).start()

    barrier = pltpu.get_barrier_semaphore()
    for k in range(1, PEERS):
        dev = plane_dev(*plane_id(k % 2, (k // 2) % 2, (c + k // 4) % 2))
        pl.semaphore_signal(barrier, inc=1, device_id=dev, device_id_type=MESH)

    @pl.when(z > 0)
    def _():
        pl.semaphore_signal(barrier, inc=1, device_id={"data": z - 1}, device_id_type=MESH)

    @pl.when(z < NZ - 1)
    def _():
        pl.semaphore_signal(barrier, inc=1, device_id={"data": z + 1}, device_id_type=MESH)

    @pl.when(outer)
    def _():
        pl.semaphore_wait(barrier, PEERS)

    @pl.when(inner)
    def _():
        pl.semaphore_wait(barrier, PEERS + 1)

    @pl.loop(0, n_chunk)
    def _(j):
        for m in range(3):
            w_local(j, m).wait()

    @pl.when(is_a)
    def _():
        @pl.when(outer)
        def _():
            own_outer()

        @pl.when(inner)
        def _():
            for j in range(AHEAD):
                light_own(j)
                heavy_own(j)

    tri = (lax.broadcasted_iota(jnp.int32, (blk, blk), 0) < lax.broadcasted_iota(jnp.int32, (blk, blk), 1)).astype(jnp.float32).astype(jnp.bfloat16)
    eye = lax.broadcasted_iota(jnp.int32, (blk, blk), 0) == lax.broadcasted_iota(jnp.int32, (blk, blk), 1)
    running = jnp.zeros((16, 1), jnp.float32)
    for b in range(n_blk):
        ids = idx_ref[:, b * blk:(b + 1) * blk]
        ids = (ids // 2 % 2) * 4 + (ids // 4) * 2 + ids % 2
        one_hot = (lax.broadcasted_iota(jnp.int32, (16, blk), 0) == ids).astype(jnp.float32)
        before = jnp.dot(one_hot.astype(jnp.bfloat16), tri, preferred_element_type=jnp.float32) + running
        slot = jnp.sum(one_hot * before, axis=0, keepdims=True)
        running = running + jnp.sum(one_hot, axis=1, keepdims=True)
        row = jnp.where(slot < cap, ids.astype(jnp.float32) * cap + slot, -1.0)
        dest[b:b + 1, :] = row.astype(jnp.int32)
        cols[b, :, 0:1] = jnp.sum(jnp.where(eye, row, 0.0), axis=1, keepdims=True)
        cols[b, :, 1:2] = jnp.sum(jnp.where(eye, gate_ref[:, b * blk:(b + 1) * blk], 0.0), axis=1, keepdims=True)

    @pl.loop(0, n_blk)
    def _(b):
        x_load(b).wait()

    def tok_copy(e, dev):
        return pltpu.make_async_remote_copy(
            src_ref=sendb.at[e], dst_ref=recv.at[me], send_sem=tok_send.at[e], recv_sem=tok_recv.at[me],
            device_id=dev, device_id_type=MESH)

    def tok_sent():
        for k in range(1, PEERS):
            peer = plane_id(k % 2, (k // 2) % 2, (c + k // 4) % 2)
            tok_copy(plane_num(*peer), plane_dev(*peer)).wait_send()

    @pl.loop(0, PEERS)
    def _(k):
        kk = k % 4
        peer = plane_id((kk + 1) % 2, ((kk + 1) // 2) % 2, k // 4)
        e = plane_num(*peer)
        slots = lax.broadcasted_iota(jnp.int32, (cap, blk), 0) + e * cap

        def pick(b):
            hot = (slots == dest[pl.ds(b, 1), :]).astype(jnp.float32).astype(jnp.bfloat16)
            return jnp.dot(hot, back[b, 0:blk, :], preferred_element_type=jnp.float32)

        acc[0] = pick(0)

        @pl.loop(1, n_blk - 1)
        def _(b):
            acc[0] += pick(b)

        rows = (acc[0] + pick(n_blk - 1)).astype(jnp.bfloat16)

        @pl.when(e == me)
        def _():
            recv[me] = rows

        @pl.when(e != me)
        def _():
            sendb[e] = rows

            tok_copy(e, plane_dev(*peer)).start()

        def at(step):
            return pl.when(jnp.logical_and(a_inner, k == step))

        @at(1)
        def _():
            light_end(0)
            light_own(3)

        @at(2)
        def _():
            light_end(1)
            light_own(4)
            heavy_mate(0)
            heavy_mate(1)
            heavy_own(3)

        @at(3)
        def _():
            light_end(2)
            light_own(5)

        @at(4)
        def _():
            light_end(3)
            heavy_mate(2)
            heavy_far(0)
            heavy_own(4)

        @at(5)
        def _():
            light_end(4)

        @at(6)
        def _():
            light_end(5)
            heavy_mate(3)
            heavy_far(1)
            heavy_own(5)

        @pl.when(jnp.logical_and(jnp.logical_and(is_a, outer), k == 6))
        def _():
            go(sent_outer, 0)

    for k in range(1, PEERS):
        dev = plane_dev(*plane_id(k % 2, (k // 2) % 2, (c + k // 4) % 2))
        pl.semaphore_signal(ready_sem, inc=1, device_id=dev, device_id_type=MESH)

    @pl.when(outer)
    def _():
        pl.semaphore_signal(ready_sem, inc=1, device_id={"data": inward}, device_id_type=MESH)

    @pl.loop(0, n_src)
    def _(s):
        acc[s] = jnp.zeros((cap, d_model), jnp.float32)

    def tok_arrived(s):
        pltpu.make_async_remote_copy(
            src_ref=sendb.at[0], dst_ref=recv.at[s], send_sem=tok_send.at[0], recv_sem=tok_recv.at[s],
            device_id={"data": inward}, device_id_type=MESH).wait_recv()

    @pl.when(a_inner)
    def _():
        heavy_mate(4)
        heavy_far(2)

    @pl.when(c == 1)
    def _():
        pl.semaphore_wait(go_sem.at[0], 1)

        @pl.when(outer)
        def _():
            own_outer()

        @pl.when(inner)
        def _():
            @pl.loop(0, n_chunk)
            def _(j):
                light_own(j)
                light_end(j)

    for k in range(1, PEERS):
        peer = plane_id(k % 2, (k // 2) % 2, (c + k // 4) % 2)
        s = plane_num(*peer)
        tok_arrived(s)

    def moved_copy(i):
        return pltpu.make_async_remote_copy(
            src_ref=recv.at[plane_num(1 - x, 1 - y, i)], dst_ref=recv.at[n_src + i], send_sem=relay_send.at[i],
            recv_sem=tok_recv.at[n_src + i], device_id={"data": inward}, device_id_type=MESH)

    @pl.when(b_outer)
    def _():
        for i in range(2):
            moved_copy(i).start()

    @pl.when(a_inner)
    def _():
        heavy_mate(5)

    @pl.when(is_b)
    def _():
        tok_sent()

    @pl.when(b_inner)
    def _():
        for owner in (mate, far):
            for m in range(3):
                w_copy(0, owner, m, True, end).wait_recv()

    def ffn(j, s):
        rows = recv[s]
        g = jnp.dot(rows, wg_buf[j], preferred_element_type=jnp.float32)
        u = jnp.dot(rows, wu_buf[j], preferred_element_type=jnp.float32)
        h = (g * jax.nn.sigmoid(g) * u).astype(jnp.bfloat16)
        return lax.dot_general(h, wd_buf[j], (((1,), (1,)), ((), ())), preferred_element_type=jnp.float32)

    def piece_of(ref, e, q):
        return ref.at[e, pl.ds(edges[q], edges[q + 1] - edges[q]), :]

    def returned(e, qs, wanted):
        @pl.when(wanted)
        def _():
            for q in qs:
                pltpu.make_async_remote_copy(
                    src_ref=piece_of(back, e, q), dst_ref=piece_of(back, e, q), send_sem=ret_send.at[e, q],
                    recv_sem=ret_recv.at[e, q], device_id={"data": inward}, device_id_type=MESH).wait_recv()

    def put_back(b, target, rows):
        hot = (target.astype(jnp.float32) == cols[b, :, 0:1]).astype(jnp.float32).astype(jnp.bfloat16)
        return jnp.dot(hot, rows.reshape(target.shape[1], d_model), preferred_element_type=jnp.float32)

    def first_half(k):
        e = 2 * ((y + k) % 2)
        for dx in range(2):
            returned(e + dx, pieces, e + dx != me)
        target = lax.broadcasted_iota(jnp.int32, (1, 2 * cap), 1) + e * cap

        @pl.loop(0, n_blk)
        def _(b):
            got = put_back(b, target, back[pl.ds(e, 2)])
            if k == 1:
                got += sendb[b, 0:blk, :].astype(jnp.float32)
            sendb[b, 0:blk, :] = got.astype(jnp.bfloat16)

    def own_chip():
        returned(4, pieces, is_a)
        target = lax.broadcasted_iota(jnp.int32, (1, cap), 1) + (4 + 2 * y + x) * cap

        @pl.loop(0, n_blk)
        def _(b):
            got = put_back(b, target, back[4]) + sendb[b, 0:blk, :].astype(jnp.float32)
            sendb[b, 0:blk, :] = got.astype(jnp.bfloat16)

    def others(q):
        rows = edges[q + 1] - edges[q]
        for e in range(5, 8):
            returned(e, (q,), p >= 0)
        col = lax.broadcasted_iota(jnp.int32, (1, 3 * rows), 1)
        i = col // rows
        expert = 4 + 2 * ((y + (i + 1) // 2) % 2) + (x + 1 - i % 2) % 2
        return expert * cap + edges[q] + col % rows, slice(edges[q], edges[q + 1])

    def skipped(s):
        return jnp.logical_and(b_outer, s % 4 == 2 * (1 - y) + 1 - x)

    def before_chunk(j):
        @pl.when(outer)
        def _():
            end_wait(j)

    @pl.loop(0, n_chunk - 1)
    def _(j):
        before_chunk(j)

        @pl.loop(0, n_src)
        def _(s):
            @pl.when(jnp.logical_not(skipped(s)))
            def _():
                acc[s] += ffn(j, s)

            @pl.when(jnp.logical_and(b_inner, jnp.logical_and(j == 0, s == 3)))
            def _():
                pl.semaphore_wait(go_sem.at[1], 1)
                for owner in (z, mate, far):
                    pass_on(0, owner, True, False)
                heavy_all(1)

        @pl.when(jnp.logical_and(a_inner, j == 0))
        def _():
            heavy_far(3)
            heavy_far(4)
            go(sent_light, 0)

        @pl.when(jnp.logical_and(a_inner, j == 1))
        def _():
            heavy_far(5)

        @pl.when(jnp.logical_and(a_inner, j == 2))
        def _():
            go(sent_heavy, 1)

        @pl.when(jnp.logical_and(b_inner, j < 4))
        def _():
            heavy_all(j + 2)

        @pl.when(jnp.logical_and(b_outer, j == 2))
        def _():
            first_half(0)

        @pl.when(jnp.logical_and(b_outer, j == 3))
        def _():
            first_half(1)

    def relay_copy(i):
        return pltpu.make_async_remote_copy(
            src_ref=recv.at[n_src + i], dst_ref=relay_hbm, send_sem=relay_send.at[i], recv_sem=relay_recv,
            device_id=plane_dev(1 - x, 1 - y, i), device_id_type=MESH)

    @pl.when(b_inner)
    def _():
        @pl.loop(0, 2)
        def _(i):
            tok_arrived(n_src + i)
            acc[n_src] = ffn(0, n_src + i)

            @pl.loop(1, n_chunk)
            def _(j):
                acc[n_src] += ffn(j, n_src + i)

            recv[n_src + i] = acc[n_src].astype(jnp.bfloat16)
            relay_copy(i).start()

    before_chunk(n_chunk - 1)

    @pl.when(is_a)
    def _():
        tok_sent()

    @pl.when(outer)
    def _():
        pl.semaphore_wait(ready_sem, PEERS - 1)

    @pl.when(inner)
    def _():
        pl.semaphore_wait(ready_sem, PEERS)

    def back_slot(peer):
        return (1 - c) * me + c * (4 + (x + peer[0]) % 2 + 2 * ((y + peer[1]) % 2))

    def ret_copy(peer, q):
        d = back_slot(peer)
        return pltpu.make_async_remote_copy(
            src_ref=piece_of(recv, plane_num(*peer), q), dst_ref=piece_of(back, d, q), send_sem=ret_send.at[plane_num(*peer), q],
            recv_sem=ret_recv.at[d, q], device_id=plane_dev(*peer), device_id_type=MESH)

    def ret_peer(r):
        q, rr = r // 4, r % 4
        return plane_id((1 - q) * ((rr + 1) % 2) + q * (1 - rr // 2), (1 - q) * (rr % 2) + q * (1 - rr // 2), (c + rr // 2 + q * rr) % 2)

    def ret_needed(s):
        return jnp.logical_and(s != me, jnp.logical_not(skipped(s)))

    @pl.loop(0, PEERS)
    def _(r):
        peer = ret_peer(r)
        s = plane_num(*peer)

        @pl.when(jnp.logical_not(skipped(s)))
        def _():
            rows = (acc[s] + ffn(n_chunk - 1, s)).astype(jnp.bfloat16)

            @pl.when(s == me)
            def _():
                back[back_slot(peer)] = rows

            @pl.when(s != me)
            def _():
                recv[s] = rows
                ret_copy(peer, 0).start()

    for q in pieces[1:]:
        @pl.loop(0, PEERS)
        def _(r):
            peer = ret_peer(r)

            @pl.when(ret_needed(plane_num(*peer)))
            def _():
                ret_copy(peer, q).start()

    def fwd_copy(q):
        return pltpu.make_async_remote_copy(
            src_ref=relay_hbm.at[pl.ds(edges[q], edges[q + 1] - edges[q]), :], dst_ref=piece_of(back, 7, q), send_sem=fwd_send.at[q],
            recv_sem=ret_recv.at[7, q], device_id={"data": end}, device_id_type=MESH)

    def relay():
        pltpu.make_async_remote_copy(
            src_ref=recv.at[0], dst_ref=relay_hbm, send_sem=relay_send.at[0], recv_sem=relay_recv,
            device_id={"data": mate}, device_id_type=MESH).wait_recv()

        @pl.when(is_b)
        def _():
            @pl.loop(0, n_chunk)
            def _(j):
                sent_heavy(j)

            pl.semaphore_signal(go_sem.at[2], inc=1, device_id={"expert": p - 1}, device_id_type=MESH)

        @pl.when(is_a)
        def _():
            pl.semaphore_wait(go_sem.at[2], 1)

        for q in pieces:
            fwd_copy(q).start()

    @pl.when(jnp.logical_not(b_outer))
    def _():
        first_half(0)

        @pl.when(b_inner)
        def _():
            relay()

        first_half(1)

        @pl.when(a_inner)
        def _():
            relay()

    for h in range(2):
        x_again(0, h).start()

    own_chip()

    def middle(q):
        target, piece = others(q)

        @pl.loop(0, n_blk)
        def _(b):
            got = put_back(b, target, back[5:8, piece, :]) + sendb[b, 0:blk, :].astype(jnp.float32)
            sendb[b, 0:blk, :] = got.astype(jnp.bfloat16)

    for q in pieces[:-1]:
        middle(q)

    target, piece = others(pieces[-1])

    def out_copy(b):
        return pltpu.make_async_copy(sendb.at[b, pl.ds(0, blk), :], x_rows(out_hbm, b), out_sem.at[b])

    @pl.loop(0, n_blk)
    def _(b):
        mixed = (put_back(b, target, back[5:8, piece, :]) + sendb[b, 0:blk, :].astype(jnp.float32)) * cols[b, :, 1:2]
        for h in range(2):
            part = slice(h * half, h * half + half)
            x_again(b, h).wait()
            sendb[b, part, :] = (x_buf[h].astype(jnp.float32) + mixed[part]).astype(jnp.bfloat16)

            @pl.when(b + 1 < n_blk)
            def _():
                x_again(b + 1, h).start()

        out_copy(b).start()

    @pl.loop((n_chunk - 1) * (1 - c), n_chunk)
    def _(j):
        @pl.when(outer)
        def _():
            sent_outer(j)

        @pl.when(inner)
        def _():
            sent_light(j)

    @pl.when(a_inner)
    def _():
        sent_heavy(n_chunk - 1)

    @pl.when(b_inner)
    def _():
        for i in range(2):
            relay_copy(i).wait_send()

    @pl.when(b_outer)
    def _():
        for i in range(2):
            moved_copy(i).wait_send()

    @pl.when(inner)
    def _():
        for q in pieces:
            fwd_copy(q).wait_send()

    @pl.loop(0, PEERS)
    def _(r):
        peer = ret_peer(r)
        s = plane_num(*peer)

        @pl.when(ret_needed(s))
        def _():
            for q in pieces:
                ret_copy(peer, q).wait_send()

    @pl.loop(0, n_blk)
    def _(b):
        out_copy(b).wait()


def solution(mesh):
    n_group = mesh.shape["expert"]
    tok_spec = P(("rep", "expert", "data"), None)
    wide_spec = P("expert", "data", None)
    down_spec = P("expert", None, "data")

    def device_step(x_loc, idx_loc, gate_loc, wg_loc, wu_loc, wd_loc):
        tok_rows, d_model = x_loc.shape
        top_k = idx_loc.shape[1]
        n_exp = wg_loc.shape[0] * n_group
        ffn = wg_loc.shape[2]
        cap = capacity_rows(tok_rows, top_k, n_exp)
        blk = tok_rows // PEERS
        f_chunk = ffn // CHUNKS
        any_spec = pl.BlockSpec(memory_space=pl.ANY)
        vmem_spec = pl.BlockSpec(memory_space=pltpu.VMEM)
        dma = pltpu.SemaphoreType.DMA
        return pl.pallas_call(
            moe_kernel,
            out_shape=(jax.ShapeDtypeStruct((tok_rows, d_model), jnp.bfloat16), jax.ShapeDtypeStruct((cap, d_model), jnp.bfloat16)),
            in_specs=[any_spec, vmem_spec, vmem_spec, any_spec, any_spec, any_spec],
            out_specs=(any_spec, any_spec),
            scratch_shapes=[
                pltpu.VMEM((CHUNKS, d_model, f_chunk), jnp.bfloat16),
                pltpu.VMEM((CHUNKS, d_model, f_chunk), jnp.bfloat16),
                pltpu.VMEM((CHUNKS, d_model, f_chunk), jnp.bfloat16),
                pltpu.VMEM((PEERS + 2, cap, d_model), jnp.bfloat16),
                pltpu.VMEM((PEERS, cap, d_model), jnp.bfloat16),
                pltpu.VMEM((PEERS, cap, d_model), jnp.bfloat16),
                pltpu.VMEM((PEERS + 1, cap, d_model), jnp.float32),
                pltpu.VMEM((2, blk // 2, d_model), jnp.bfloat16),
                pltpu.VMEM((PEERS, blk), jnp.int32),
                pltpu.VMEM((PEERS, blk, 2), jnp.float32),
                dma((CHUNKS, NZ, 3)), dma((CHUNKS, NZ, 3)), dma((CHUNKS, NZ, 3)),
                dma((PEERS + 2,)), dma((PEERS,)), dma((PEERS, 3)), dma((PEERS, 3)), dma, dma((2,)), dma((3,)),
                dma((PEERS,)), dma((PEERS,)), pltpu.SemaphoreType.REGULAR((3,)), pltpu.SemaphoreType.REGULAR,
            ],
            compiler_params=pltpu.CompilerParams(collective_id=0, has_side_effects=True, vmem_limit_bytes=VMEM_BYTES),
        )(x_loc, idx_loc.T, gate_loc.T, wg_loc, wu_loc, wd_loc.transpose(0, 2, 1))[0]

    return jax.shard_map(device_step, mesh=mesh, in_specs=(tok_spec, tok_spec, tok_spec, wide_spec, wide_spec, down_spec), out_specs=tok_spec, check_vma=False)
```

```python
import functools

import jax
import jax.numpy as jnp
from jax import lax
from jax.experimental import pallas as pl
from jax.experimental.pallas import tpu as pltpu
from jax.sharding import PartitionSpec as P

MESH = pl.DeviceIdType.MESH
CHUNKS = 6
NZ = 4
PEERS = 8
AHEAD = 3
VMEM_BYTES = 67_000_000


def capacity_rows(tok_rows, top_k, n_exp):
    return max(8, ((5 * top_k * tok_rows) // (4 * n_exp) + 7) // 8 * 8)


def slot_edges(cap):
    return 0, cap * 3 // 5, cap


def moe_kernel(x_hbm, idx_ref, gate_ref, wg_hbm, wu_hbm, wd_hbm, out_hbm, relay_hbm,
               wg_buf, wu_buf, wd_buf, recv, sendb, back, acc, dest, cols,
               w_recv, w_light, w_heavy, tok_recv, tok_send, ret_recv, ret_send, relay_recv, relay_send, fwd_send,
               x_sem, out_sem, go_sem, ready_sem):
    n_src, cap, d_model = back.shape
    edges = slot_edges(cap)
    pieces = range(len(edges) - 1)
    n_blk, blk, _ = cols.shape
    n_chunk, _, f_chunk = wg_buf.shape
    shard = d_model // NZ

    x = lax.axis_index("rep")
    z = lax.axis_index("data")
    p = lax.axis_index("expert")
    y, c = p // 2, p % 2
    me = 4 * c + 2 * y + x
    is_a = c == 0
    inner = jnp.logical_and(z > 0, z < NZ - 1)
    outer = jnp.logical_or(z == 0, z == NZ - 1)
    is_b = c == 1
    a_inner = jnp.logical_and(is_a, inner)
    b_inner = jnp.logical_and(is_b, inner)
    b_outer = jnp.logical_and(is_b, outer)
    inward = (z + 3) // 3

    def plane_id(dx, dy, cc):
        return (x + dx) % 2, (y + dy) % 2, cc

    def plane_dev(px, py, pc):
        return {"rep": px, "expert": 2 * py + pc}

    def plane_num(px, py, pc):
        return 4 * pc + 2 * py + px

    def w_view(j, s, m):
        return (wg_buf, wu_buf, wd_buf)[m].at[j, pl.ds(s * shard, shard), :]

    def w_local(j, m):
        src = (wg_hbm, wu_hbm, wd_hbm)[m].at[x, :, pl.ds(pl.multiple_of(j * f_chunk, f_chunk), f_chunk)]
        return pltpu.make_async_copy(src, w_view(j, z, m), w_recv.at[j, z, m])

    def w_copy(j, s, m, heavy, dev):
        view = w_view(j, s, m)
        return pltpu.make_async_remote_copy(
            src_ref=view, dst_ref=view, send_sem=(w_heavy if heavy else w_light).at[j, s, m], recv_sem=w_recv.at[j, s, m],
            device_id={"data": dev}, device_id_type=MESH)

    end, far, mate = 3 * (z - 1), 3 * (2 - z), 3 - z

    def pass_on(j, s, heavy, arrives=True):
        for m in range(3):
            cp = w_copy(j, s, m, heavy, end if heavy else mate)
            if arrives:
                cp.wait_recv()
            cp.start()

    def light_own(j):
        pass_on(j, z, False, False)

    def light_end(j):
        pass_on(j, end, False)

    def heavy_own(j):
        pass_on(j, z, True, False)

    def heavy_mate(j):
        pass_on(j, mate, True)

    def heavy_far(j):
        pass_on(j, far, True)

    def heavy_all(j):
        heavy_own(j)
        heavy_mate(j)
        heavy_far(j)

    def own_outer():
        @pl.loop(0, n_chunk)
        def _(j):
            for m in range(3):
                w_copy(j, z, m, False, inward).start()

    def end_wait(j):
        for d in range(1, NZ):
            for m in range(3):
                w_copy(j, (z + d) % NZ, m, False, inward).wait_recv()

    def sent(j, shards, heavy):
        for s in shards:
            for m in range(3):
                w_copy(j, s, m, heavy, (z + 1) % NZ).wait_send()

    def sent_outer(j):
        sent(j, (z,), False)

    def sent_light(j):
        sent(j, (z, end), False)

    def sent_heavy(j):
        sent(j, (z, mate, far), True)

    def go(done, heavy):
        @pl.loop(0, n_chunk - 1)
        def _(j):
            done(j)

        pl.semaphore_signal(go_sem.at[heavy], inc=1, device_id={"expert": p + 1}, device_id_type=MESH)

    def x_rows(ref, b):
        return ref.at[pl.ds(pl.multiple_of(b * blk, blk), blk), :]

    def x_load(b):
        return pltpu.make_async_copy(x_rows(x_hbm, b), back.at[b, pl.ds(0, blk), :], x_sem.at[b])

    def x_again(b):
        return pltpu.make_async_copy(x_rows(x_hbm, b), back.at[b % 4, pl.ds(0, blk), :], x_sem.at[b % 4])

    @pl.loop(0, n_chunk)
    def _(j):
        for m in range(3):
            w_local(j, m).start()

    @pl.loop(0, n_blk)
    def _(b):
        x_load(b).start()

    barrier = pltpu.get_barrier_semaphore()
    for k in range(1, PEERS):
        dev = plane_dev(*plane_id(k % 2, (k // 2) % 2, (c + k // 4) % 2))
        pl.semaphore_signal(barrier, inc=1, device_id=dev, device_id_type=MESH)

    @pl.when(z > 0)
    def _():
        pl.semaphore_signal(barrier, inc=1, device_id={"data": z - 1}, device_id_type=MESH)

    @pl.when(z < NZ - 1)
    def _():
        pl.semaphore_signal(barrier, inc=1, device_id={"data": z + 1}, device_id_type=MESH)

    @pl.when(outer)
    def _():
        pl.semaphore_wait(barrier, PEERS)

    @pl.when(inner)
    def _():
        pl.semaphore_wait(barrier, PEERS + 1)

    @pl.loop(0, n_chunk)
    def _(j):
        for m in range(3):
            w_local(j, m).wait()

    @pl.when(is_a)
    def _():
        @pl.when(outer)
        def _():
            own_outer()

        @pl.when(inner)
        def _():
            for j in range(AHEAD):
                light_own(j)
                heavy_own(j)

    tri = (lax.broadcasted_iota(jnp.int32, (blk, blk), 0) < lax.broadcasted_iota(jnp.int32, (blk, blk), 1)).astype(jnp.float32).astype(jnp.bfloat16)
    eye = lax.broadcasted_iota(jnp.int32, (blk, blk), 0) == lax.broadcasted_iota(jnp.int32, (blk, blk), 1)
    running = jnp.zeros((16, 1), jnp.float32)
    for b in range(n_blk):
        ids = idx_ref[:, b * blk:(b + 1) * blk]
        ids = (ids // 2 % 2) * 4 + (ids // 4) * 2 + ids % 2
        one_hot = (lax.broadcasted_iota(jnp.int32, (16, blk), 0) == ids).astype(jnp.float32)
        before = jnp.dot(one_hot.astype(jnp.bfloat16), tri, preferred_element_type=jnp.float32) + running
        slot = jnp.sum(one_hot * before, axis=0, keepdims=True)
        running = running + jnp.sum(one_hot, axis=1, keepdims=True)
        row = jnp.where(slot < cap, ids.astype(jnp.float32) * cap + slot, -1.0)
        dest[b:b + 1, :] = row.astype(jnp.int32)
        cols[b, :, 0:1] = jnp.sum(jnp.where(eye, row, 0.0), axis=1, keepdims=True)
        cols[b, :, 1:2] = jnp.sum(jnp.where(eye, gate_ref[:, b * blk:(b + 1) * blk], 0.0), axis=1, keepdims=True)

    @pl.loop(0, n_blk)
    def _(b):
        x_load(b).wait()

    def tok_copy(e, dev):
        return pltpu.make_async_remote_copy(
            src_ref=sendb.at[e], dst_ref=recv.at[me], send_sem=tok_send.at[e], recv_sem=tok_recv.at[me],
            device_id=dev, device_id_type=MESH)

    def tok_sent():
        for k in range(1, PEERS):
            peer = plane_id(k % 2, (k // 2) % 2, (c + k // 4) % 2)
            tok_copy(plane_num(*peer), plane_dev(*peer)).wait_send()

    @pl.loop(0, PEERS)
    def _(k):
        kk = k % 4
        peer = plane_id((kk + 1) % 2, ((kk + 1) // 2) % 2, k // 4)
        e = plane_num(*peer)
        slots = lax.broadcasted_iota(jnp.int32, (cap, blk), 0) + e * cap

        def pick(b):
            hot = (slots == dest[pl.ds(b, 1), :]).astype(jnp.float32).astype(jnp.bfloat16)
            return jnp.dot(hot, back[b, 0:blk, :], preferred_element_type=jnp.float32)

        acc[0] = pick(0)

        @pl.loop(1, n_blk - 1)
        def _(b):
            acc[0] += pick(b)

        rows = (acc[0] + pick(n_blk - 1)).astype(jnp.bfloat16)

        @pl.when(e == me)
        def _():
            recv[me] = rows

        @pl.when(e != me)
        def _():
            sendb[e] = rows

            tok_copy(e, plane_dev(*peer)).start()

        def at(step):
            return pl.when(jnp.logical_and(a_inner, k == step))

        @at(1)
        def _():
            light_end(0)
            light_own(3)

        @at(2)
        def _():
            light_end(1)
            light_own(4)
            heavy_mate(0)
            heavy_mate(1)
            heavy_own(3)

        @at(3)
        def _():
            light_end(2)
            light_own(5)

        @at(4)
        def _():
            light_end(3)
            heavy_mate(2)
            heavy_far(0)
            heavy_own(4)

        @at(5)
        def _():
            light_end(4)

        @at(6)
        def _():
            light_end(5)
            heavy_mate(3)
            heavy_far(1)
            heavy_own(5)

        @pl.when(jnp.logical_and(jnp.logical_and(is_a, outer), k == 6))
        def _():
            go(sent_outer, 0)

    for k in range(1, PEERS):
        dev = plane_dev(*plane_id(k % 2, (k // 2) % 2, (c + k // 4) % 2))
        pl.semaphore_signal(ready_sem, inc=1, device_id=dev, device_id_type=MESH)

    @pl.when(outer)
    def _():
        pl.semaphore_signal(ready_sem, inc=1, device_id={"data": inward}, device_id_type=MESH)

    @pl.loop(0, n_src)
    def _(s):
        acc[s] = jnp.zeros((cap, d_model), jnp.float32)

    def tok_arrived(s):
        pltpu.make_async_remote_copy(
            src_ref=sendb.at[0], dst_ref=recv.at[s], send_sem=tok_send.at[0], recv_sem=tok_recv.at[s],
            device_id={"data": inward}, device_id_type=MESH).wait_recv()

    @pl.when(a_inner)
    def _():
        heavy_mate(4)
        heavy_far(2)

    @pl.when(c == 1)
    def _():
        pl.semaphore_wait(go_sem.at[0], 1)

        @pl.when(outer)
        def _():
            own_outer()

        @pl.when(inner)
        def _():
            @pl.loop(0, n_chunk)
            def _(j):
                light_own(j)
                light_end(j)

    for k in range(1, PEERS):
        peer = plane_id(k % 2, (k // 2) % 2, (c + k // 4) % 2)
        s = plane_num(*peer)
        tok_arrived(s)

    def moved_copy(i):
        return pltpu.make_async_remote_copy(
            src_ref=recv.at[plane_num(1 - x, 1 - y, i)], dst_ref=recv.at[n_src + i], send_sem=relay_send.at[i],
            recv_sem=tok_recv.at[n_src + i], device_id={"data": inward}, device_id_type=MESH)

    @pl.when(b_outer)
    def _():
        for i in range(2):
            moved_copy(i).start()

    @pl.when(a_inner)
    def _():
        heavy_mate(5)

    @pl.when(is_b)
    def _():
        tok_sent()

    @pl.when(b_inner)
    def _():
        for owner in (mate, far):
            for m in range(3):
                w_copy(0, owner, m, True, end).wait_recv()

    def ffn(j, s):
        rows = recv[s]
        g = jnp.dot(rows, wg_buf[j], preferred_element_type=jnp.float32)
        u = jnp.dot(rows, wu_buf[j], preferred_element_type=jnp.float32)
        h = (g * jax.nn.sigmoid(g) * u).astype(jnp.bfloat16)
        return lax.dot_general(h, wd_buf[j], (((1,), (1,)), ((), ())), preferred_element_type=jnp.float32)

    def piece_of(ref, e, q):
        return ref.at[e, pl.ds(edges[q], edges[q + 1] - edges[q]), :]

    def returned(e, qs, wanted):
        @pl.when(wanted)
        def _():
            for q in qs:
                pltpu.make_async_remote_copy(
                    src_ref=piece_of(back, e, q), dst_ref=piece_of(back, e, q), send_sem=ret_send.at[e, q],
                    recv_sem=ret_recv.at[e, q], device_id={"data": inward}, device_id_type=MESH).wait_recv()

    def put_back(b, target, rows):
        hot = (target.astype(jnp.float32) == cols[b, :, 0:1]).astype(jnp.float32).astype(jnp.bfloat16)
        return jnp.dot(hot, rows.reshape(target.shape[1], d_model), preferred_element_type=jnp.float32)

    def first_half(k):
        e = 2 * ((y + k) % 2)
        for dx in range(2):
            returned(e + dx, pieces, e + dx != me)
        target = lax.broadcasted_iota(jnp.int32, (1, 2 * cap), 1) + e * cap

        @pl.loop(0, n_blk)
        def _(b):
            got = put_back(b, target, back[pl.ds(e, 2)])
            if k == 1:
                got += sendb[b, 0:blk, :].astype(jnp.float32)
            sendb[b, 0:blk, :] = got.astype(jnp.bfloat16)

    def own_chip():
        returned(4, pieces, is_a)
        target = lax.broadcasted_iota(jnp.int32, (1, cap), 1) + (4 + 2 * y + x) * cap

        @pl.loop(0, n_blk)
        def _(b):
            got = put_back(b, target, back[4]) + sendb[b, 0:blk, :].astype(jnp.float32)
            sendb[b, 0:blk, :] = got.astype(jnp.bfloat16)

    def others(q):
        rows = edges[q + 1] - edges[q]
        for e in range(5, 8):
            returned(e, (q,), p >= 0)
        col = lax.broadcasted_iota(jnp.int32, (1, 3 * rows), 1)
        i = col // rows
        expert = 4 + 2 * ((y + (i + 1) // 2) % 2) + (x + 1 - i % 2) % 2
        return expert * cap + edges[q] + col % rows, slice(edges[q], edges[q + 1])

    def skipped(s):
        return jnp.logical_and(b_outer, s % 4 == 2 * (1 - y) + 1 - x)

    def before_chunk(j):
        @pl.when(outer)
        def _():
            end_wait(j)

    @pl.loop(0, n_chunk - 1)
    def _(j):
        before_chunk(j)

        @pl.loop(0, n_src)
        def _(s):
            @pl.when(jnp.logical_not(skipped(s)))
            def _():
                acc[s] += ffn(j, s)

            @pl.when(jnp.logical_and(b_inner, jnp.logical_and(j == 0, s == 3)))
            def _():
                pl.semaphore_wait(go_sem.at[1], 1)
                for owner in (z, mate, far):
                    pass_on(0, owner, True, False)
                heavy_all(1)

        @pl.when(jnp.logical_and(a_inner, j == 0))
        def _():
            heavy_far(3)
            heavy_far(4)
            go(sent_light, 0)

        @pl.when(jnp.logical_and(a_inner, j == 1))
        def _():
            heavy_far(5)

        @pl.when(jnp.logical_and(a_inner, j == 2))
        def _():
            go(sent_heavy, 1)

        @pl.when(jnp.logical_and(b_inner, j < 4))
        def _():
            heavy_all(j + 2)

        @pl.when(jnp.logical_and(b_outer, j == 2))
        def _():
            first_half(0)

        @pl.when(jnp.logical_and(b_outer, j == 3))
        def _():
            first_half(1)

    def relay_copy(i):
        return pltpu.make_async_remote_copy(
            src_ref=recv.at[n_src + i], dst_ref=relay_hbm, send_sem=relay_send.at[i], recv_sem=relay_recv,
            device_id=plane_dev(1 - x, 1 - y, i), device_id_type=MESH)

    @pl.when(b_inner)
    def _():
        @pl.loop(0, 2)
        def _(i):
            tok_arrived(n_src + i)
            acc[n_src] = ffn(0, n_src + i)

            @pl.loop(1, n_chunk)
            def _(j):
                acc[n_src] += ffn(j, n_src + i)

            recv[n_src + i] = acc[n_src].astype(jnp.bfloat16)
            relay_copy(i).start()

    before_chunk(n_chunk - 1)

    @pl.when(is_a)
    def _():
        tok_sent()

    @pl.when(outer)
    def _():
        pl.semaphore_wait(ready_sem, PEERS - 1)

    @pl.when(inner)
    def _():
        pl.semaphore_wait(ready_sem, PEERS)

    def back_slot(peer):
        return (1 - c) * me + c * (4 + (x + peer[0]) % 2 + 2 * ((y + peer[1]) % 2))

    def ret_copy(peer, q):
        d = back_slot(peer)
        return pltpu.make_async_remote_copy(
            src_ref=piece_of(recv, plane_num(*peer), q), dst_ref=piece_of(back, d, q), send_sem=ret_send.at[plane_num(*peer), q],
            recv_sem=ret_recv.at[d, q], device_id=plane_dev(*peer), device_id_type=MESH)

    def ret_peer(r):
        third = (r + 5) // 8
        r = r + 4 * ((r + 6) // 8 - third) - third + (r + 1) // 8
        q, rr = r // 4, r % 4
        return plane_id((1 - q) * ((rr + 1) % 2) + q * (1 - rr // 2), (1 - q) * (rr % 2) + q * (1 - rr // 2), (c + rr // 2 + q * rr) % 2)

    def ret_needed(s):
        return jnp.logical_and(s != me, jnp.logical_not(skipped(s)))

    @pl.loop(0, PEERS)
    def _(r):
        peer = ret_peer(r)
        s = plane_num(*peer)

        @pl.when(jnp.logical_not(skipped(s)))
        def _():
            rows = (acc[s] + ffn(n_chunk - 1, s)).astype(jnp.bfloat16)

            @pl.when(s == me)
            def _():
                back[back_slot(peer)] = rows

            @pl.when(s != me)
            def _():
                recv[s] = rows
                ret_copy(peer, 0).start()

    for q in pieces[1:]:
        @pl.loop(0, PEERS)
        def _(r):
            peer = ret_peer(r)

            @pl.when(ret_needed(plane_num(*peer)))
            def _():
                ret_copy(peer, q).start()

    def fwd_copy(q):
        return pltpu.make_async_remote_copy(
            src_ref=relay_hbm.at[pl.ds(edges[q], edges[q + 1] - edges[q]), :], dst_ref=piece_of(back, 7, q), send_sem=fwd_send.at[q],
            recv_sem=ret_recv.at[7, q], device_id={"data": end}, device_id_type=MESH)

    def relay():
        pltpu.make_async_remote_copy(
            src_ref=recv.at[0], dst_ref=relay_hbm, send_sem=relay_send.at[0], recv_sem=relay_recv,
            device_id={"data": mate}, device_id_type=MESH).wait_recv()

        @pl.when(is_b)
        def _():
            @pl.loop(0, n_chunk)
            def _(j):
                sent_heavy(j)

            pl.semaphore_signal(go_sem.at[2], inc=1, device_id={"expert": p - 1}, device_id_type=MESH)

        @pl.when(is_a)
        def _():
            pl.semaphore_wait(go_sem.at[2], 1)

        for q in pieces:
            fwd_copy(q).start()

    @pl.when(jnp.logical_not(b_outer))
    def _():
        first_half(0)

        @pl.when(b_inner)
        def _():
            relay()

        first_half(1)

        @pl.when(a_inner)
        def _():
            relay()

    for b in range(4):
        x_again(b).start()

    own_chip()

    def middle(q):
        target, piece = others(q)

        @pl.loop(0, n_blk)
        def _(b):
            got = put_back(b, target, back[5:8, piece, :]) + sendb[b, 0:blk, :].astype(jnp.float32)
            sendb[b, 0:blk, :] = got.astype(jnp.bfloat16)

    for q in pieces[:-1]:
        middle(q)

    target, piece = others(pieces[-1])

    def out_copy(b):
        return pltpu.make_async_copy(sendb.at[b, pl.ds(0, blk), :], x_rows(out_hbm, b), out_sem.at[b])

    @pl.loop(0, n_blk)
    def _(b):
        mixed = (put_back(b, target, back[5:8, piece, :]) + sendb[b, 0:blk, :].astype(jnp.float32)) * cols[b, :, 1:2]
        x_again(b).wait()
        sendb[b, 0:blk, :] = (back[b % 4, 0:blk, :].astype(jnp.float32) + mixed).astype(jnp.bfloat16)

        @pl.when(b + 4 < n_blk)
        def _():
            x_again(b + 4).start()

        out_copy(b).start()

    @pl.loop((n_chunk - 1) * (1 - c), n_chunk)
    def _(j):
        @pl.when(outer)
        def _():
            sent_outer(j)

        @pl.when(inner)
        def _():
            sent_light(j)

    @pl.when(a_inner)
    def _():
        sent_heavy(n_chunk - 1)

    @pl.when(b_inner)
    def _():
        for i in range(2):
            relay_copy(i).wait_send()

    @pl.when(b_outer)
    def _():
        for i in range(2):
            moved_copy(i).wait_send()

    @pl.when(inner)
    def _():
        for q in pieces:
            fwd_copy(q).wait_send()

    @pl.loop(0, PEERS)
    def _(r):
        peer = ret_peer(r)
        s = plane_num(*peer)

        @pl.when(ret_needed(s))
        def _():
            for q in pieces:
                ret_copy(peer, q).wait_send()

    @pl.loop(0, n_blk)
    def _(b):
        out_copy(b).wait()


def solution(mesh):
    n_group = mesh.shape["expert"]
    tok_spec = P(("rep", "expert", "data"), None)
    wide_spec = P("expert", "data", None)
    down_spec = P("expert", None, "data")

    def device_step(x_loc, idx_loc, gate_loc, wg_loc, wu_loc, wd_loc):
        tok_rows, d_model = x_loc.shape
        top_k = idx_loc.shape[1]
        n_exp = wg_loc.shape[0] * n_group
        ffn = wg_loc.shape[2]
        cap = capacity_rows(tok_rows, top_k, n_exp)
        blk = tok_rows // PEERS
        f_chunk = ffn // CHUNKS
        any_spec = pl.BlockSpec(memory_space=pl.ANY)
        vmem_spec = pl.BlockSpec(memory_space=pltpu.VMEM)
        dma = pltpu.SemaphoreType.DMA
        return pl.pallas_call(
            moe_kernel,
            out_shape=(jax.ShapeDtypeStruct((tok_rows, d_model), jnp.bfloat16), jax.ShapeDtypeStruct((cap, d_model), jnp.bfloat16)),
            in_specs=[any_spec, vmem_spec, vmem_spec, any_spec, any_spec, any_spec],
            out_specs=(any_spec, any_spec),
            scratch_shapes=[
                pltpu.VMEM((CHUNKS, d_model, f_chunk), jnp.bfloat16),
                pltpu.VMEM((CHUNKS, d_model, f_chunk), jnp.bfloat16),
                pltpu.VMEM((CHUNKS, d_model, f_chunk), jnp.bfloat16),
                pltpu.VMEM((PEERS + 2, cap, d_model), jnp.bfloat16),
                pltpu.VMEM((PEERS, cap, d_model), jnp.bfloat16),
                pltpu.VMEM((PEERS, cap, d_model), jnp.bfloat16),
                pltpu.VMEM((PEERS + 1, cap, d_model), jnp.float32),
                pltpu.VMEM((PEERS, blk), jnp.int32),
                pltpu.VMEM((PEERS, blk, 2), jnp.float32),
                dma((CHUNKS, NZ, 3)), dma((CHUNKS, NZ, 3)), dma((CHUNKS, NZ, 3)),
                dma((PEERS + 2,)), dma((PEERS,)), dma((PEERS, 2)), dma((PEERS, 2)), dma, dma((2,)), dma((2,)),
                dma((PEERS,)), dma((PEERS,)), pltpu.SemaphoreType.REGULAR((3,)), pltpu.SemaphoreType.REGULAR,
            ],
            compiler_params=pltpu.CompilerParams(collective_id=0, has_side_effects=True, vmem_limit_bytes=VMEM_BYTES),
        )(x_loc, idx_loc.T, gate_loc.T, wg_loc, wu_loc, wd_loc.transpose(0, 2, 1))[0]

    return jax.shard_map(device_step, mesh=mesh, in_specs=(tok_spec, tok_spec, tok_spec, wide_spec, wide_spec, down_spec), out_specs=tok_spec, check_vma=False)
```

```python
import functools

import jax
import jax.numpy as jnp
from jax import lax
from jax.experimental import pallas as pl
from jax.experimental.pallas import tpu as pltpu
from jax.sharding import PartitionSpec as P

MESH = pl.DeviceIdType.MESH
CHUNKS = 6
NZ = 4
PEERS = 8
AHEAD = 3
VMEM_BYTES = 67_000_000


def capacity_rows(tok_rows, top_k, n_exp):
    return max(8, ((5 * top_k * tok_rows) // (4 * n_exp) + 7) // 8 * 8)


def slot_edges(cap):
    return 0, cap * 3 // 5, cap


def moe_kernel(x_hbm, idx_ref, gate_ref, wg_hbm, wu_hbm, wd_hbm, out_hbm, relay_hbm,
               wg_buf, wu_buf, wd_buf, recv, sendb, back, acc, dest, cols,
               w_recv, w_light, w_heavy, tok_recv, tok_send, ret_recv, ret_send, relay_recv, relay_send, fwd_send,
               x_sem, out_sem, go_sem, ready_sem):
    n_src, cap, d_model = back.shape
    edges = slot_edges(cap)
    pieces = range(len(edges) - 1)
    n_blk, blk, _ = cols.shape
    n_chunk, _, f_chunk = wg_buf.shape
    shard = d_model // NZ

    x = lax.axis_index("rep")
    z = lax.axis_index("data")
    p = lax.axis_index("expert")
    y, c = p // 2, p % 2
    me = 4 * c + 2 * y + x
    is_a = c == 0
    inner = jnp.logical_and(z > 0, z < NZ - 1)
    outer = jnp.logical_or(z == 0, z == NZ - 1)
    is_b = c == 1
    a_inner = jnp.logical_and(is_a, inner)
    b_inner = jnp.logical_and(is_b, inner)
    b_outer = jnp.logical_and(is_b, outer)
    inward = (z + 3) // 3

    def plane_id(dx, dy, cc):
        return (x + dx) % 2, (y + dy) % 2, cc

    def plane_dev(px, py, pc):
        return {"rep": px, "expert": 2 * py + pc}

    def plane_num(px, py, pc):
        return 4 * pc + 2 * py + px

    def w_view(j, s, m):
        return (wg_buf, wu_buf, wd_buf)[m].at[j, pl.ds(s * shard, shard), :]

    def w_local(j, m):
        src = (wg_hbm, wu_hbm, wd_hbm)[m].at[x, :, pl.ds(pl.multiple_of(j * f_chunk, f_chunk), f_chunk)]
        return pltpu.make_async_copy(src, w_view(j, z, m), w_recv.at[j, z, m])

    def w_copy(j, s, m, heavy, dev, role=0):
        view = w_view(j, s, m)
        return pltpu.make_async_remote_copy(
            src_ref=view, dst_ref=view, send_sem=(w_heavy if heavy else w_light).at[j, role], recv_sem=w_recv.at[j, s, m],
            device_id={"data": dev}, device_id_type=MESH)

    end, far, mate = 3 * (z - 1), 3 * (2 - z), 3 - z

    def pass_on(j, s, heavy, role, arrives=True):
        for m in range(3):
            cp = w_copy(j, s, m, heavy, end if heavy else mate, role)
            if arrives:
                cp.wait_recv()
            cp.start()

    def light_own(j):
        pass_on(j, z, False, 0, False)

    def light_end(j):
        pass_on(j, end, False, 1)

    def heavy_own(j):
        pass_on(j, z, True, 0, False)

    def heavy_mate(j):
        pass_on(j, mate, True, 1)

    def heavy_far(j):
        pass_on(j, far, True, 2)

    def heavy_all(j):
        heavy_own(j)
        heavy_mate(j)
        heavy_far(j)

    def own_outer():
        @pl.loop(0, n_chunk)
        def _(j):
            for m in range(3):
                w_copy(j, z, m, False, inward).start()

    def end_wait(j):
        for d in range(1, NZ):
            for m in range(3):
                w_copy(j, (z + d) % NZ, m, False, inward).wait_recv()

    def sent(j, roles, heavy):
        rows = wg_buf.at[j, pl.ds(0, 3 * shard), :]
        for role in range(roles):
            pltpu.make_async_remote_copy(
                src_ref=rows, dst_ref=rows, send_sem=(w_heavy if heavy else w_light).at[j, role], recv_sem=w_recv.at[j, 0, 0],
                device_id={"data": inward}, device_id_type=MESH).wait_send()

    def sent_outer(j):
        sent(j, 1, False)

    def sent_light(j):
        sent(j, 2, False)

    def sent_heavy(j):
        sent(j, 3, True)

    def go(done, heavy):
        @pl.loop(0, n_chunk - 1)
        def _(j):
            done(j)

        pl.semaphore_signal(go_sem.at[heavy], inc=1, device_id={"expert": p + 1}, device_id_type=MESH)

    def x_rows(ref, b):
        return ref.at[pl.ds(pl.multiple_of(b * blk, blk), blk), :]

    def x_load(b):
        return pltpu.make_async_copy(x_rows(x_hbm, b), back.at[b, pl.ds(0, blk), :], x_sem.at[b])

    def x_again(b):
        return pltpu.make_async_copy(x_rows(x_hbm, b), back.at[b % 4, pl.ds(0, blk), :], x_sem.at[b % 4])

    @pl.loop(0, n_chunk)
    def _(j):
        for m in range(3):
            w_local(j, m).start()

    @pl.loop(0, n_blk)
    def _(b):
        x_load(b).start()

    barrier = pltpu.get_barrier_semaphore()
    for k in range(1, PEERS):
        dev = plane_dev(*plane_id(k % 2, (k // 2) % 2, (c + k // 4) % 2))
        pl.semaphore_signal(barrier, inc=1, device_id=dev, device_id_type=MESH)

    @pl.when(z > 0)
    def _():
        pl.semaphore_signal(barrier, inc=1, device_id={"data": z - 1}, device_id_type=MESH)

    @pl.when(z < NZ - 1)
    def _():
        pl.semaphore_signal(barrier, inc=1, device_id={"data": z + 1}, device_id_type=MESH)

    @pl.when(outer)
    def _():
        pl.semaphore_wait(barrier, PEERS)

    @pl.when(inner)
    def _():
        pl.semaphore_wait(barrier, PEERS + 1)

    @pl.loop(0, n_chunk)
    def _(j):
        for m in range(3):
            w_local(j, m).wait()

    @pl.when(is_a)
    def _():
        @pl.when(outer)
        def _():
            own_outer()

        @pl.when(inner)
        def _():
            for j in range(AHEAD):
                light_own(j)
                heavy_own(j)

    tri = (lax.broadcasted_iota(jnp.int32, (blk, blk), 0) < lax.broadcasted_iota(jnp.int32, (blk, blk), 1)).astype(jnp.float32).astype(jnp.bfloat16)
    eye = lax.broadcasted_iota(jnp.int32, (blk, blk), 0) == lax.broadcasted_iota(jnp.int32, (blk, blk), 1)
    running = jnp.zeros((16, 1), jnp.float32)
    for b in range(n_blk):
        ids = idx_ref[:, b * blk:(b + 1) * blk]
        ids = (ids // 2 % 2) * 4 + (ids // 4) * 2 + ids % 2
        one_hot = (lax.broadcasted_iota(jnp.int32, (16, blk), 0) == ids).astype(jnp.float32)
        before = jnp.dot(one_hot.astype(jnp.bfloat16), tri, preferred_element_type=jnp.float32) + running
        slot = jnp.sum(one_hot * before, axis=0, keepdims=True)
        running = running + jnp.sum(one_hot, axis=1, keepdims=True)
        row = jnp.where(slot < cap, ids.astype(jnp.float32) * cap + slot, -1.0)
        dest[b:b + 1, :] = row.astype(jnp.int32)
        cols[b, :, 0:1] = jnp.sum(jnp.where(eye, row, 0.0), axis=1, keepdims=True)
        cols[b, :, 1:2] = jnp.sum(jnp.where(eye, gate_ref[:, b * blk:(b + 1) * blk], 0.0), axis=1, keepdims=True)

    @pl.loop(0, n_blk)
    def _(b):
        x_load(b).wait()

    def tok_copy(e, dev):
        return pltpu.make_async_remote_copy(
            src_ref=sendb.at[e], dst_ref=recv.at[me], send_sem=tok_send.at[e], recv_sem=tok_recv.at[me],
            device_id=dev, device_id_type=MESH)

    def tok_sent():
        for k in range(1, PEERS):
            peer = plane_id(k % 2, (k // 2) % 2, (c + k // 4) % 2)
            tok_copy(plane_num(*peer), plane_dev(*peer)).wait_send()

    @pl.loop(0, PEERS)
    def _(k):
        kk = k % 4
        peer = plane_id((kk + 1) % 2, ((kk + 1) // 2) % 2, k // 4)
        e = plane_num(*peer)
        slots = lax.broadcasted_iota(jnp.int32, (cap, blk), 0) + e * cap

        def pick(b):
            hot = (slots == dest[pl.ds(b, 1), :]).astype(jnp.float32).astype(jnp.bfloat16)
            return jnp.dot(hot, back[b, 0:blk, :], preferred_element_type=jnp.float32)

        acc[0] = pick(0)

        @pl.loop(1, n_blk - 1)
        def _(b):
            acc[0] += pick(b)

        rows = (acc[0] + pick(n_blk - 1)).astype(jnp.bfloat16)

        @pl.when(e == me)
        def _():
            recv[me] = rows

        @pl.when(e != me)
        def _():
            sendb[e] = rows

            tok_copy(e, plane_dev(*peer)).start()

        def at(step):
            return pl.when(jnp.logical_and(a_inner, k == step))

        @at(1)
        def _():
            light_end(0)
            light_own(3)

        @at(2)
        def _():
            light_end(1)
            light_own(4)
            heavy_mate(0)
            heavy_mate(1)
            heavy_own(3)

        @at(3)
        def _():
            light_end(2)
            light_own(5)

        @at(4)
        def _():
            light_end(3)
            heavy_mate(2)
            heavy_far(0)
            heavy_own(4)

        @at(5)
        def _():
            light_end(4)

        @at(6)
        def _():
            light_end(5)
            heavy_mate(3)
            heavy_far(1)
            heavy_own(5)

        @pl.when(jnp.logical_and(jnp.logical_and(is_a, outer), k == 6))
        def _():
            go(sent_outer, 0)

    for k in range(1, PEERS):
        dev = plane_dev(*plane_id(k % 2, (k // 2) % 2, (c + k // 4) % 2))
        pl.semaphore_signal(ready_sem, inc=1, device_id=dev, device_id_type=MESH)

    @pl.when(outer)
    def _():
        pl.semaphore_signal(ready_sem, inc=1, device_id={"data": inward}, device_id_type=MESH)

    @pl.loop(0, n_src)
    def _(s):
        acc[s] = jnp.zeros((cap, d_model), jnp.float32)

    def tok_arrived(s):
        pltpu.make_async_remote_copy(
            src_ref=sendb.at[0], dst_ref=recv.at[s], send_sem=tok_send.at[0], recv_sem=tok_recv.at[s],
            device_id={"data": inward}, device_id_type=MESH).wait_recv()

    @pl.when(a_inner)
    def _():
        heavy_mate(4)
        heavy_far(2)

    @pl.when(c == 1)
    def _():
        pl.semaphore_wait(go_sem.at[0], 1)

        @pl.when(outer)
        def _():
            own_outer()

        @pl.when(inner)
        def _():
            @pl.loop(0, n_chunk)
            def _(j):
                light_own(j)
                light_end(j)

    for k in range(1, PEERS):
        peer = plane_id(k % 2, (k // 2) % 2, (c + k // 4) % 2)
        s = plane_num(*peer)
        tok_arrived(s)

    def moved_copy(i):
        return pltpu.make_async_remote_copy(
            src_ref=recv.at[plane_num(1 - x, 1 - y, i)], dst_ref=recv.at[n_src + i], send_sem=relay_send.at[i],
            recv_sem=tok_recv.at[n_src + i], device_id={"data": inward}, device_id_type=MESH)

    @pl.when(b_outer)
    def _():
        for i in range(2):
            moved_copy(i).start()

    @pl.when(a_inner)
    def _():
        heavy_mate(5)

    @pl.when(is_b)
    def _():
        tok_sent()

    @pl.when(b_inner)
    def _():
        for owner in (mate, far):
            for m in range(3):
                w_copy(0, owner, m, True, end).wait_recv()

    def ffn(j, s):
        rows = recv[s]
        g = jnp.dot(rows, wg_buf[j], preferred_element_type=jnp.float32)
        u = jnp.dot(rows, wu_buf[j], preferred_element_type=jnp.float32)
        h = (g * jax.nn.sigmoid(g) * u).astype(jnp.bfloat16)
        return lax.dot_general(h, wd_buf[j], (((1,), (1,)), ((), ())), preferred_element_type=jnp.float32)

    def piece_of(ref, e, q):
        return ref.at[e, pl.ds(edges[q], edges[q + 1] - edges[q]), :]

    def returned(e, qs, wanted):
        @pl.when(wanted)
        def _():
            for q in qs:
                pltpu.make_async_remote_copy(
                    src_ref=piece_of(back, e, q), dst_ref=piece_of(back, e, q), send_sem=ret_send.at[e, q],
                    recv_sem=ret_recv.at[e, q], device_id={"data": inward}, device_id_type=MESH).wait_recv()

    def put_back(b, target, rows):
        hot = (target.astype(jnp.float32) == cols[b, :, 0:1]).astype(jnp.float32).astype(jnp.bfloat16)
        return jnp.dot(hot, rows.reshape(target.shape[1], d_model), preferred_element_type=jnp.float32)

    def first_half(k):
        e = 2 * ((y + k) % 2)
        for dx in range(2):
            returned(e + dx, pieces, e + dx != me)
        target = lax.broadcasted_iota(jnp.int32, (1, 2 * cap), 1) + e * cap

        @pl.loop(0, n_blk)
        def _(b):
            got = put_back(b, target, back[pl.ds(e, 2)])
            if k == 1:
                got += sendb[b, 0:blk, :].astype(jnp.float32)
            sendb[b, 0:blk, :] = got.astype(jnp.bfloat16)

    def own_chip():
        returned(4, pieces, is_a)
        target = lax.broadcasted_iota(jnp.int32, (1, cap), 1) + (4 + 2 * y + x) * cap

        @pl.loop(0, n_blk)
        def _(b):
            got = put_back(b, target, back[4]) + sendb[b, 0:blk, :].astype(jnp.float32)
            sendb[b, 0:blk, :] = got.astype(jnp.bfloat16)

    def others(q):
        rows = edges[q + 1] - edges[q]
        for e in range(5, 8):
            returned(e, (q,), p >= 0)
        col = lax.broadcasted_iota(jnp.int32, (1, 3 * rows), 1)
        i = col // rows
        expert = 4 + 2 * ((y + (i + 1) // 2) % 2) + (x + 1 - i % 2) % 2
        return expert * cap + edges[q] + col % rows, slice(edges[q], edges[q + 1])

    def skipped(s):
        return jnp.logical_and(b_outer, s % 4 == 2 * (1 - y) + 1 - x)

    def before_chunk(j):
        @pl.when(outer)
        def _():
            end_wait(j)

    @pl.loop(0, n_chunk - 1)
    def _(j):
        before_chunk(j)

        @pl.loop(0, n_src)
        def _(s):
            @pl.when(jnp.logical_not(skipped(s)))
            def _():
                acc[s] += ffn(j, s)

            @pl.when(jnp.logical_and(b_inner, jnp.logical_and(j == 0, s == 3)))
            def _():
                pl.semaphore_wait(go_sem.at[1], 1)
                for role, owner in enumerate((z, mate, far)):
                    pass_on(0, owner, True, role, False)
                heavy_all(1)

        @pl.when(jnp.logical_and(a_inner, j == 0))
        def _():
            heavy_far(3)
            heavy_far(4)
            go(sent_light, 0)

        @pl.when(jnp.logical_and(a_inner, j == 1))
        def _():
            heavy_far(5)

        @pl.when(jnp.logical_and(a_inner, j == 2))
        def _():
            go(sent_heavy, 1)

        @pl.when(jnp.logical_and(b_inner, j < 4))
        def _():
            heavy_all(j + 2)

        @pl.when(jnp.logical_and(b_outer, j == 2))
        def _():
            first_half(0)

        @pl.when(jnp.logical_and(b_outer, j == 3))
        def _():
            first_half(1)

    def relay_copy(i):
        return pltpu.make_async_remote_copy(
            src_ref=recv.at[n_src + i], dst_ref=relay_hbm, send_sem=relay_send.at[i], recv_sem=relay_recv,
            device_id=plane_dev(1 - x, 1 - y, i), device_id_type=MESH)

    @pl.when(b_inner)
    def _():
        @pl.loop(0, 2)
        def _(i):
            tok_arrived(n_src + i)
            acc[n_src] = ffn(0, n_src + i)

            @pl.loop(1, n_chunk)
            def _(j):
                acc[n_src] += ffn(j, n_src + i)

            recv[n_src + i] = acc[n_src].astype(jnp.bfloat16)
            relay_copy(i).start()

    before_chunk(n_chunk - 1)

    @pl.when(is_a)
    def _():
        tok_sent()

    @pl.when(outer)
    def _():
        pl.semaphore_wait(ready_sem, PEERS - 1)

    @pl.when(inner)
    def _():
        pl.semaphore_wait(ready_sem, PEERS)

    def back_slot(peer):
        return (1 - c) * me + c * (4 + (x + peer[0]) % 2 + 2 * ((y + peer[1]) % 2))

    def ret_copy(peer, q):
        d = back_slot(peer)
        return pltpu.make_async_remote_copy(
            src_ref=piece_of(recv, plane_num(*peer), q), dst_ref=piece_of(back, d, q), send_sem=ret_send.at[plane_num(*peer), q],
            recv_sem=ret_recv.at[d, q], device_id=plane_dev(*peer), device_id_type=MESH)

    def ret_peer(r):
        third = (r + 5) // 8
        r = r + 4 * ((r + 6) // 8 - third) - third + (r + 1) // 8
        q, rr = r // 4, r % 4
        return plane_id((1 - q) * ((rr + 1) % 2) + q * (1 - rr // 2), (1 - q) * (rr % 2) + q * (1 - rr // 2), (c + rr // 2 + q * rr) % 2)

    def ret_needed(s):
        return jnp.logical_and(s != me, jnp.logical_not(skipped(s)))

    @pl.loop(0, PEERS)
    def _(r):
        peer = ret_peer(r)
        s = plane_num(*peer)

        @pl.when(jnp.logical_not(skipped(s)))
        def _():
            rows = (acc[s] + ffn(n_chunk - 1, s)).astype(jnp.bfloat16)

            @pl.when(s == me)
            def _():
                back[back_slot(peer)] = rows

            @pl.when(s != me)
            def _():
                recv[s] = rows
                ret_copy(peer, 0).start()

    for q in pieces[1:]:
        @pl.loop(0, PEERS)
        def _(r):
            peer = ret_peer(r)

            @pl.when(ret_needed(plane_num(*peer)))
            def _():
                ret_copy(peer, q).start()

    def fwd_copy(q):
        return pltpu.make_async_remote_copy(
            src_ref=relay_hbm.at[pl.ds(edges[q], edges[q + 1] - edges[q]), :], dst_ref=piece_of(back, 7, q), send_sem=fwd_send.at[q],
            recv_sem=ret_recv.at[7, q], device_id={"data": end}, device_id_type=MESH)

    def relay():
        pltpu.make_async_remote_copy(
            src_ref=recv.at[0], dst_ref=relay_hbm, send_sem=relay_send.at[0], recv_sem=relay_recv,
            device_id={"data": mate}, device_id_type=MESH).wait_recv()

        @pl.when(is_b)
        def _():
            @pl.loop(0, n_chunk)
            def _(j):
                sent_heavy(j)

            pl.semaphore_signal(go_sem.at[2], inc=1, device_id={"expert": p - 1}, device_id_type=MESH)

        @pl.when(is_a)
        def _():
            pl.semaphore_wait(go_sem.at[2], 1)

        for q in pieces:
            fwd_copy(q).start()

    @pl.when(jnp.logical_not(b_outer))
    def _():
        first_half(0)

        @pl.when(b_inner)
        def _():
            relay()

        first_half(1)

        @pl.when(a_inner)
        def _():
            relay()

    for b in range(4):
        x_again(b).start()

    own_chip()

    def middle(q):
        target, piece = others(q)

        @pl.loop(0, n_blk)
        def _(b):
            got = put_back(b, target, back[5:8, piece, :]) + sendb[b, 0:blk, :].astype(jnp.float32)
            sendb[b, 0:blk, :] = got.astype(jnp.bfloat16)

    for q in pieces[:-1]:
        middle(q)

    target, piece = others(pieces[-1])

    def out_copy(b):
        return pltpu.make_async_copy(sendb.at[b, pl.ds(0, blk), :], x_rows(out_hbm, b), out_sem.at[b])

    @pl.loop(0, n_blk)
    def _(b):
        mixed = (put_back(b, target, back[5:8, piece, :]) + sendb[b, 0:blk, :].astype(jnp.float32)) * cols[b, :, 1:2]
        x_again(b).wait()
        sendb[b, 0:blk, :] = (back[b % 4, 0:blk, :].astype(jnp.float32) + mixed).astype(jnp.bfloat16)

        @pl.when(b + 4 < n_blk)
        def _():
            x_again(b + 4).start()

        out_copy(b).start()

    @pl.loop((n_chunk - 1) * (1 - c), n_chunk)
    def _(j):
        @pl.when(outer)
        def _():
            sent_outer(j)

        @pl.when(inner)
        def _():
            sent_light(j)

    @pl.when(a_inner)
    def _():
        sent_heavy(n_chunk - 1)

    @pl.when(b_inner)
    def _():
        for i in range(2):
            relay_copy(i).wait_send()

    @pl.when(b_outer)
    def _():
        for i in range(2):
            moved_copy(i).wait_send()

    @pl.when(inner)
    def _():
        for q in pieces:
            fwd_copy(q).wait_send()

    @pl.loop(0, PEERS)
    def _(r):
        peer = ret_peer(r)
        s = plane_num(*peer)

        @pl.when(ret_needed(s))
        def _():
            for q in pieces:
                ret_copy(peer, q).wait_send()

    @pl.loop(0, n_blk)
    def _(b):
        out_copy(b).wait()


def solution(mesh):
    n_group = mesh.shape["expert"]
    tok_spec = P(("rep", "expert", "data"), None)
    wide_spec = P("expert", "data", None)
    down_spec = P("expert", None, "data")

    def device_step(x_loc, idx_loc, gate_loc, wg_loc, wu_loc, wd_loc):
        tok_rows, d_model = x_loc.shape
        top_k = idx_loc.shape[1]
        n_exp = wg_loc.shape[0] * n_group
        ffn = wg_loc.shape[2]
        cap = capacity_rows(tok_rows, top_k, n_exp)
        blk = tok_rows // PEERS
        f_chunk = ffn // CHUNKS
        any_spec = pl.BlockSpec(memory_space=pl.ANY)
        vmem_spec = pl.BlockSpec(memory_space=pltpu.VMEM)
        dma = pltpu.SemaphoreType.DMA
        return pl.pallas_call(
            moe_kernel,
            out_shape=(jax.ShapeDtypeStruct((tok_rows, d_model), jnp.bfloat16), jax.ShapeDtypeStruct((cap, d_model), jnp.bfloat16)),
            in_specs=[any_spec, vmem_spec, vmem_spec, any_spec, any_spec, any_spec],
            out_specs=(any_spec, any_spec),
            scratch_shapes=[
                pltpu.VMEM((CHUNKS, d_model, f_chunk), jnp.bfloat16),
                pltpu.VMEM((CHUNKS, d_model, f_chunk), jnp.bfloat16),
                pltpu.VMEM((CHUNKS, d_model, f_chunk), jnp.bfloat16),
                pltpu.VMEM((PEERS + 2, cap, d_model), jnp.bfloat16),
                pltpu.VMEM((PEERS, cap, d_model), jnp.bfloat16),
                pltpu.VMEM((PEERS, cap, d_model), jnp.bfloat16),
                pltpu.VMEM((PEERS + 1, cap, d_model), jnp.float32),
                pltpu.VMEM((PEERS, blk), jnp.int32),
                pltpu.VMEM((PEERS, blk, 2), jnp.float32),
                dma((CHUNKS, NZ, 3)), dma((CHUNKS, 2)), dma((CHUNKS, 3)),
                dma((PEERS + 2,)), dma((PEERS,)), dma((PEERS, 2)), dma((PEERS, 2)), dma, dma((2,)), dma((2,)),
                dma((PEERS,)), dma((PEERS,)), pltpu.SemaphoreType.REGULAR((3,)), pltpu.SemaphoreType.REGULAR,
            ],
            compiler_params=pltpu.CompilerParams(collective_id=0, has_side_effects=True, vmem_limit_bytes=VMEM_BYTES),
        )(x_loc, idx_loc.T, gate_loc.T, wg_loc, wu_loc, wd_loc.transpose(0, 2, 1))[0]

    return jax.shard_map(device_step, mesh=mesh, in_specs=(tok_spec, tok_spec, tok_spec, wide_spec, wide_spec, down_spec), out_specs=tok_spec, check_vma=False)
```
